32 devices in a mesh: lat: 4 (over z), lon: 8 (over y, x, core).
Axes of the slice: x: 2, y: 2, z: 4, core: 2. Of those that a mesh axis runs over, the one named last changes fastest.
Arguments:
- fields: bfloat16 [3, 512, 32, 384], P(None, ('lat', 'lon')), may hold values from -6 to 6
- weights: bfloat16 [3, 1024, 8, 32, 128], P(None, ('lat', 'lon')), may hold values from -0.5 to 0.5
- pair_slots: int32 [3, 1024, 8], P(None, ('lat', 'lon')), may hold values from 0 to 15
- pair_counts: int32 [3, 1024], P(None, ('lat', 'lon')), may hold values from 1 to 8
- requests: int32 [3, 32, 16], replicated, may hold values from 0 to 511, as said below
- eofs: bfloat16 [200, 131072], P(None, ('lat', 'lon')), may hold values from -0.015625 to 0.015625
Outputs:
- pcs: float32 [200, 1152], P(None, ('lat', 'lon'))
The draws below stay inside these ranges and needn't reach their ends.
Inputs may be any that keep to these rules, and one draw needn't show every extreme that they name: requests[g, d] lists 16 distinct source tiles for grid g and device d (d = lat index * lon devices + lon index); source tile j lies on device j // 16; all of them lie on devices with d's lat index whose lon index is d's own or one of its two cyclic neighbours, at most 8 on any one device, and exactly 8 on some device for every g and d. `pair_slots`: only entries with p < pair_counts[g, t] are used.
All inputs are finite; a program needn't handle non-finite values.
Results may differ from the reference program's by a relative error of at most 0.0029.
Values may be sent and summed in bfloat16 or wider, within the bound.
No kernel may reach another device: no remote copies, remote signals or barrier semaphores. Data moves between devices by JAX's collectives and lax.ppermute only.
A program may use at most 128 MiB of HBM per device.

```python
import jax
import jax.numpy as jnp
from jax import lax

EOFS = 200
TT = 128
TS = 32
MAXP = 8
MONTHS = 24
GRIDS = 3
MODELS_G = 16
TILES_DEV = 32
STILES_DEV = 16
REQ = 16
CAP = 8
GCOLS = 384
TARGET_TILES = 1024
CELLS = 131072
SRC_TILES = 512
N_LAT = 4
N_LON = 8


def draw_requests(key, part):
    device_total = N_LAT * N_LON
    keys_all = jax.random.split(key, 4)
    heavy = jax.random.randint(keys_all[0], (GRIDS, device_total), 0, 3)
    offsets = jax.random.randint(keys_all[1], (GRIDS, device_total, 3), 0, STILES_DEV)
    perm_keys = jax.random.split(keys_all[2], GRIDS * device_total)
    others = jax.vmap(lambda single: jax.random.permutation(single, 2 * CAP)[:REQ - CAP])(perm_keys)
    others = others.reshape(GRIDS, device_total, REQ - CAP)
    order_keys = jax.random.split(keys_all[3], GRIDS * device_total)
    orders = jax.vmap(lambda single: jax.random.permutation(single, REQ))(order_keys).reshape(GRIDS, device_total, REQ)
    first_rel = jnp.broadcast_to(heavy[:, :, None], (GRIDS, device_total, CAP))
    first_rank = jnp.broadcast_to(jnp.arange(CAP, dtype=jnp.int32)[None, None, :], (GRIDS, device_total, CAP))
    other_index = others // CAP
    other_rel = other_index + (other_index >= heavy[:, :, None]).astype(jnp.int32)
    other_rank = others % CAP
    relative = jnp.concatenate([first_rel, other_rel], axis=2).astype(jnp.int32)
    ranking = jnp.concatenate([first_rank, other_rank], axis=2).astype(jnp.int32)
    chosen_offset = jnp.take_along_axis(offsets, relative, axis=2)
    local_tile = (chosen_offset + ranking) % STILES_DEV
    devices = jnp.arange(device_total, dtype=jnp.int32)[None, :, None]
    band = devices // N_LON
    sector = (devices % N_LON + relative - 1 + N_LON) % N_LON
    tiles = (band * N_LON + sector) * STILES_DEV + local_tile
    tiles = jnp.take_along_axis(tiles, orders, axis=2)
    return tiles.astype(jnp.int32)


def with_ends(drawn, key, smallest, top_value):
    longest = drawn.shape.index(max(drawn.shape))
    spots = []
    for shift in (0, 1):
        where = [jax.random.randint(jax.random.fold_in(key, axis), (), 0, length) for axis, length in enumerate(drawn.shape)]
        where[longest] = (where[longest] + shift) % drawn.shape[longest]
        spots.append(tuple(where))
    return drawn.at[spots[0]].set(smallest).at[spots[1]].set(top_value)


def levels(key, extent, cuts, low, top_value):
    factor_of = 1.0
    for position, shards_of in cuts:
        draws = jax.random.uniform(jax.random.fold_in(jax.random.fold_in(key, 6), position), (shards_of,), jnp.float32, low / len(cuts), top_value / len(cuts))
        factor_of = factor_of * jnp.repeat(jnp.exp(draws), extent[position] // shards_of).reshape((-1,) + (1,) * (len(extent) - 1 - position))
    return factor_of


def normal_values(own_key, shape, scale, most, cuts=(), kind=jnp.bfloat16):
    result = jax.random.normal(own_key, shape, jnp.float32) * scale
    if len(cuts) > 0:
        result = levels(own_key, shape, cuts, -0.22, 0.18) * result
    return jnp.clip(result, min=-most, max=most).astype(kind)


def setup_inputs(seed: int = 0) -> dict:
    keys = jax.random.split(jax.random.key(seed), 7)
    return {
        "fields": normal_values(keys[0], (GRIDS, SRC_TILES, TS, GCOLS), 1.0, 6.0, ((1, 32),)),
        "weights": normal_values(keys[1], (GRIDS, TARGET_TILES, MAXP, TS, TT), (TS * MAXP // 2) ** -0.5, 0.5, ((1, 32),)),
        "pair_slots": with_ends(jax.random.randint(keys[2], (GRIDS, TARGET_TILES, MAXP), 0, REQ), jax.random.fold_in(keys[2], 1), 0, REQ - 1).astype(jnp.int32),
        "pair_counts": with_ends(jax.random.randint(keys[3], (GRIDS, TARGET_TILES), 1, MAXP + 1), jax.random.fold_in(keys[3], 1), 1, MAXP).astype(jnp.int32),
        "requests": draw_requests(jax.random.fold_in(keys[6], 71), 0),
        "eofs": normal_values(keys[5], (EOFS, CELLS), CELLS ** -0.5, 0.015625, ((1, 32),)),
    }


def reference(fields, weights, pair_slots, pair_counts, requests, eofs):
    device_total = N_LAT * N_LON

    def one_device(running, device):
        start = device * TILES_DEV
        tile_weights = lax.dynamic_slice_in_dim(weights, start, TILES_DEV, 1)
        tile_slots = lax.dynamic_slice_in_dim(pair_slots, start, TILES_DEV, 1)
        tile_counts = lax.dynamic_slice_in_dim(pair_counts, start, TILES_DEV, 1)
        basis = lax.dynamic_slice_in_dim(eofs, start * TT, TILES_DEV * TT, 1)
        wanted = lax.dynamic_index_in_dim(requests, device, 1, keepdims=False)
        pieces = []
        for grid_id in range(GRIDS):
            tile_ids = wanted[grid_id][tile_slots[grid_id]]
            blocks = fields[grid_id][tile_ids]
            live_slots = jnp.arange(MAXP, dtype=jnp.int32)[None, :] < tile_counts[grid_id][:, None]
            masked = jnp.where(live_slots[:, :, None, None], tile_weights[grid_id], jnp.zeros((), jnp.bfloat16))
            regridded = jnp.einsum('tpsx,tpsc->txc', masked.astype(jnp.float32), blocks.astype(jnp.float32))
            by_model = regridded.reshape(TILES_DEV, TT, MODELS_G, MONTHS)
            anomaly = (by_model - jnp.mean(by_model, axis=3, keepdims=True)).astype(jnp.bfloat16)
            anomaly = anomaly.reshape(TILES_DEV * TT, MODELS_G * MONTHS)
            pieces.append(jnp.dot(basis, anomaly, preferred_element_type=jnp.float32))
        return running + jnp.concatenate(pieces, axis=1), None

    initial = jnp.zeros((EOFS, GRIDS * MODELS_G * MONTHS), jnp.float32)
    total, unused = lax.scan(one_device, initial, jnp.arange(device_total, dtype=jnp.int32))
    return total
```

```python
import functools

import jax
import jax.numpy as jnp
from jax import lax
from jax.experimental import pallas as pl
from jax.experimental.pallas import tpu as pltpu
from jax.sharding import PartitionSpec as P

MONTHS = 24
CORES = 2

SMEM = pl.BlockSpec(memory_space=pltpu.SMEM)
VMEM = pl.BlockSpec(memory_space=pltpu.VMEM)


def place():
    lon_count = lax.axis_size("lon")
    return lax.axis_index("lat"), lax.axis_index("lon"), lon_count


def pick_kernel(requests, fields, up_ref, down_ref, order):
    lat, lon, lon_count = place()
    grids, src_tiles = fields.shape[:2]
    slots = requests.shape[2]
    cap = up_ref.shape[1]
    mine = lat * lon_count + lon
    for side, out in ((1, up_ref), (lon_count - 1, down_ref)):
        other = lat * lon_count + lax.rem(lon + side, lon_count)
        for g in range(grids):
            for j in range(cap):
                order[j] = 0
            rank = jnp.int32(0)
            for r in range(slots):
                tile = requests[g, other, r]
                order[rank] = lax.rem(tile, src_tiles)
                rank += (lax.div(tile, src_tiles) == mine).astype(jnp.int32)
            for j in range(cap):
                out[g, j] = fields[g, order[j]]


def pick(requests, fields):
    grids, src_tiles, cells, columns = fields.shape
    cap = requests.shape[2] // 2
    packed = jax.ShapeDtypeStruct((grids, cap, cells, columns), fields.dtype)
    return pl.pallas_call(
        pick_kernel,
        out_shape=(packed, packed),
        in_specs=[SMEM, VMEM],
        out_specs=(VMEM, VMEM),
        scratch_shapes=[pltpu.SMEM((cap + 1,), jnp.int32)],
        name="pick",
    )(requests, fields)


def fold_kernel(src_tiles, requests, slots_ref, counts_ref, w_ref, e_ref, a_ref, where, *totals):
    step = pl.program_id(0)
    grids, tiles, depth, cells_x = w_ref.shape
    slots = requests.shape[2]
    cap = slots // 2
    pairs = slots_ref.shape[2]
    cells = depth // pairs
    eofs = e_ref.shape[0]
    lanes = a_ref.shape[2] // 2
    lat, lon, lon_count = place()
    mine = lat * lon_count + lon

    @pl.when(step == 0)
    def _():
        for total in totals:
            total[...] = jnp.zeros_like(total)
        for g in range(grids):
            ranks = [jnp.int32(0)] * 3
            for r in range(slots):
                sector = lax.div(requests[g, mine, r], src_tiles) - lat * lon_count
                relative = lax.rem(sector - lon + 1 + lon_count, lon_count)
                hits = [(relative == k).astype(jnp.int32) for k in range(3)]
                rank = sum(h * k for h, k in zip(hits, ranks))
                where[g, r] = relative * cap + rank
                ranks = [k + h for k, h in zip(ranks, hits)]

    for t in range(tiles):
        tile = step * tiles + t
        basis = e_ref[:, t * cells_x : (t + 1) * cells_x]
        parts = [
            lax.dot_general(
                w_ref[g, t], basis, (((1,), (1,)), ((), ())), preferred_element_type=jnp.float32
            )
            for g in range(grids)
        ]
        for p in range(pairs):
            for g in range(grids):
                spot = where[g, slots_ref[g, tile, p]]
                spot = jnp.where(p < counts_ref[g, tile], spot, 3 * cap)
                rows = pl.ds(pl.multiple_of(spot * cells, cells), cells)
                totals[g][rows, :] += parts[g][p * cells : (p + 1) * cells]

    @pl.when(step == pl.num_programs(0) - 1)
    def _():
        for g in range(grids):
            total = totals[g][: 3 * cap * cells, :]
            high = total.astype(jnp.bfloat16)
            low = (total - high.astype(jnp.float32)).astype(jnp.bfloat16)
            a_ref[g, :, :eofs] = high
            a_ref[g, :, lanes : lanes + eofs] = low


def fold(requests, slots, counts, weights, eofs, src_tiles):
    grids, tile_total, pairs, cells, cells_x = weights.shape
    cap = requests.shape[2] // 2
    lanes = pl.cdiv(eofs.shape[0], 128) * 128
    tiles = 4
    weights = weights.reshape(grids, tile_total, pairs * cells, cells_x)
    flops = 2 * grids * tile_total * pairs * cells * cells_x * eofs.shape[0]
    return pl.pallas_call(
        functools.partial(fold_kernel, src_tiles),
        out_shape=jax.ShapeDtypeStruct((grids, 3 * cap * cells, 2 * lanes), jnp.bfloat16),
        grid=(tile_total // tiles,),
        in_specs=[
            SMEM,
            SMEM,
            SMEM,
            pl.BlockSpec((grids, tiles, pairs * cells, cells_x), lambda i: (0, i, 0, 0)),
            pl.BlockSpec((eofs.shape[0], tiles * cells_x), lambda i: (0, i)),
        ],
        out_specs=pl.BlockSpec((grids, 3 * cap * cells, 2 * lanes), lambda i: (0, 0, 0)),
        scratch_shapes=[pltpu.SMEM((grids, 2 * cap), jnp.int32)]
        + [pltpu.VMEM(((3 * cap + 1) * cells, eofs.shape[0]), jnp.float32)] * grids,
        cost_estimate=pl.CostEstimate(
            flops=8 * flops, bytes_accessed=weights.size * 2, transcendentals=0
        ),
        name="fold",
    )(requests, slots, counts, weights, eofs)


def project_kernel(lat_count, requests, left, fields, right, a_ref, keep_ref, send_ref, order, own, whole, units):
    lat, lon, lon_count = place()
    grids, src_tiles, cells, columns = fields.shape
    slots = requests.shape[2]
    cap = slots // 2
    eofs = keep_ref.shape[2]
    lanes = a_ref.shape[2] // 2
    planes = lon_count // CORES
    rows = units.shape[1]
    mine = lat * lon_count + lon
    depth = cap * cells
    for g in range(grids):
        for j in range(cap):
            order[j] = 0
        rank = jnp.int32(0)
        for r in range(slots):
            tile = requests[g, mine, r]
            order[rank] = lax.rem(tile, src_tiles)
            rank += (lax.div(tile, src_tiles) == mine).astype(jnp.int32)
        for j in range(cap):
            own[j * cells : (j + 1) * cells, :] = fields[g, order[j]]
        total = jnp.zeros((columns, 2 * lanes), jnp.float32)
        sources = (left[g].reshape(depth, columns), own[...], right[g].reshape(depth, columns))
        for k, source in enumerate(sources):
            total += lax.dot_general(
                source,
                a_ref[g, k * depth : (k + 1) * depth, :],
                (((0,), (0,)), ((), ())),
                preferred_element_type=jnp.float32,
            )
        product = total[:, :eofs] + total[:, lanes : lanes + eofs]
        product = product.reshape(columns // MONTHS, MONTHS, eofs)
        product = product - jnp.mean(product, axis=1, keepdims=True)
        whole[g * columns : (g + 1) * columns, :] = product.reshape(columns, eofs)
    for u in range(units.shape[0]):
        units[u] = whole[u * rows : (u + 1) * rows, :]
    plane, core = lax.div(lon, CORES), lax.rem(lon, CORES)
    for c, out in ((0, keep_ref), (1, send_ref)):
        for r in range(planes):
            for q in range(lat_count):
                target = jnp.bitwise_xor(lat, q) * lon_count
                target += jnp.bitwise_xor(plane, r) * CORES + jnp.bitwise_xor(core, c)
                out[r, q * rows : (q + 1) * rows, :] = units[target]


def project(requests, left, fields, right, folded, eofs):
    lat_count, lon_count = lax.axis_size("lat"), lax.axis_size("lon")
    grids, src_tiles, cells, columns = fields.shape
    cap = requests.shape[2] // 2
    total_columns = grids * columns
    rows = total_columns // (lat_count * lon_count)
    block = jax.ShapeDtypeStruct((lon_count // CORES, lat_count * rows, eofs), jnp.float32)
    return pl.pallas_call(
        functools.partial(project_kernel, lat_count),
        out_shape=(block, block),
        in_specs=[SMEM, VMEM, VMEM, VMEM, VMEM],
        out_specs=(VMEM, VMEM),
        scratch_shapes=[
            pltpu.SMEM((cap + 1,), jnp.int32),
            pltpu.VMEM((cap * cells, columns), fields.dtype),
            pltpu.VMEM((total_columns, eofs), jnp.float32),
            pltpu.VMEM((lat_count * lon_count, rows, eofs), jnp.float32),
        ],
        name="project",
    )(requests, left, fields, right, folded)


def shards(fields, weights, pair_slots, pair_counts, requests, eofs):
    lat_count, lon_count = lax.axis_size("lat"), lax.axis_size("lon")
    planes = lon_count // CORES
    up_ring = [(i, (i + 1) % lon_count) for i in range(lon_count)]
    down_ring = [(j, i) for i, j in up_ring]
    up, down = pick(requests, fields)
    left = lax.ppermute(up, "lon", up_ring)
    right = lax.ppermute(down, "lon", down_ring)
    folded = fold(requests, pair_slots, pair_counts, weights, eofs, fields.shape[1])
    keep, send = project(requests, left, fields, right, folded, eofs.shape[0])
    pair_sum = keep + lax.ppermute(send, "lon", [(i, i ^ 1) for i in range(lon_count)])
    plane_sum = pair_sum[0]
    for r in range(1, planes):
        swap = [(i, i ^ (r * CORES)) for i in range(lon_count)]
        plane_sum = plane_sum + lax.ppermute(pair_sum[r], "lon", swap)
    rows = plane_sum.shape[0] // lat_count
    total = plane_sum[:rows]
    for q in range(1, lat_count):
        swap = [(i, i ^ q) for i in range(lat_count)]
        total = total + lax.ppermute(plane_sum[q * rows : (q + 1) * rows], "lat", swap)
    return total.T


def solution(mesh):
    return jax.shard_map(
        shards,
        mesh=mesh,
        in_specs=(
            P(None, ("lat", "lon"), None, None),
            P(None, ("lat", "lon"), None, None, None),
            P(None, ("lat", "lon"), None),
            P(None, ("lat", "lon")),
            P(),
            P(None, ("lat", "lon")),
        ),
        out_specs=P(None, ("lat", "lon")),
        check_vma=False,
    )
```

```python
import functools

import jax
import jax.numpy as jnp
from jax import lax
from jax.experimental import pallas as pl
from jax.experimental.pallas import tpu as pltpu
from jax.sharding import PartitionSpec as P

MONTHS = 24
CORES = 2
MIB = 2**20

SMEM = pl.BlockSpec(memory_space=pltpu.SMEM)
VMEM = pl.BlockSpec(memory_space=pltpu.VMEM)
HBM = pl.BlockSpec(memory_space=pl.ANY)


def grant(size):
    return pltpu.CompilerParams(vmem_limit_bytes=size * MIB)


def stay(array):
    return pltpu.with_memory_space_constraint(array, pltpu.HBM)


def place():
    lat, lon, lon_count = lax.axis_index("lat"), lax.axis_index("lon"), lax.axis_size("lon")
    core = lax.rem(lon, CORES)
    pair = lon + 1 - 2 * core
    cross = lax.rem(lon + 2 * core - 1 + lon_count, lon_count)
    return lat, lon, pair, cross, lat * lon_count, lon_count


def list_tiles(requests, order, g, reader, owner, src_tiles):
    cap = order.shape[0] - 1
    for j in range(cap):
        order[j] = 0
    rank = jnp.int32(0)
    for r in range(requests.shape[1]):
        tile = requests[g, r, reader]
        order[rank] = lax.rem(tile, src_tiles)
        rank += (lax.div(tile, src_tiles) == owner).astype(jnp.int32)


def pick_kernel(requests, fields, out_ref, order, sems):
    lat, lon, pair, cross, base, lon_count = place()
    grids, src_tiles = fields.shape[:2]
    cap = out_ref.shape[1]
    copies = []
    for g in range(grids):
        list_tiles(requests, order, g, base + cross, base + lon, src_tiles)
        for j in range(cap):
            copy = pltpu.make_async_copy(fields.at[g, order[j]], out_ref.at[g, j], sems.at[g, j])
            copy.start()
            copies.append(copy)
    for copy in copies:
        copy.wait()


def pick(requests, fields):
    grids, src_tiles, cells, columns = fields.shape
    cap = requests.shape[1] // 2
    return pl.pallas_call(
        pick_kernel,
        out_shape=jax.ShapeDtypeStruct((grids, cap, cells, columns), fields.dtype),
        in_specs=[SMEM, HBM],
        out_specs=VMEM,
        scratch_shapes=[
            pltpu.SMEM((cap + 1,), jnp.int32),
            pltpu.SemaphoreType.DMA((grids, cap)),
        ],
        compiler_params=grant(2),
        name="pick",
    )(requests, fields)


def fold_kernel(src_tiles, requests, slots_ref, counts_ref, w_ref, e_ref, a_ref, where, *totals):
    step = pl.program_id(0)
    grids, tiles, depth, cells_x = w_ref.shape
    slots = requests.shape[1]
    cap = slots // 2
    pairs = slots_ref.shape[1]
    cells = depth // pairs
    eofs = e_ref.shape[0]
    lanes = a_ref.shape[2] // 2
    lat, lon, pair, cross, base, lon_count = place()

    @pl.when(step == 0)
    def _():
        for total in totals:
            total[...] = jnp.zeros_like(total)
        for g in range(grids):
            ranks = [jnp.int32(0)] * 3
            for r in range(slots):
                owner = lax.div(requests[g, r, base + lon], src_tiles) - base
                hits = [(owner == k).astype(jnp.int32) for k in (lon, pair)]
                hits.append(1 - hits[0] - hits[1])
                where[g, r] = sum(h * (k * cap + n) for k, (h, n) in enumerate(zip(hits, ranks)))
                ranks = [n + h for n, h in zip(ranks, hits)]

    for t in range(tiles):
        tile = step * tiles + t
        basis = e_ref[:, t * cells_x : (t + 1) * cells_x]
        parts = [
            lax.dot_general(
                w_ref[g, t], basis, (((1,), (1,)), ((), ())), preferred_element_type=jnp.float32
            )
            for g in range(grids)
        ]
        for p in range(pairs):
            for g in range(grids):
                spot = where[g, slots_ref[g, p, tile]]
                spot = jnp.where(p < counts_ref[g, tile], spot, 3 * cap)
                rows = pl.ds(pl.multiple_of(spot * cells, cells), cells)
                totals[g][rows, :] += parts[g][p * cells : (p + 1) * cells]

    @pl.when(step == pl.num_programs(0) - 1)
    def _():
        for g in range(grids):
            total = totals[g][: 3 * cap * cells, :]
            high = total.astype(jnp.bfloat16)
            low = (total - high.astype(jnp.float32)).astype(jnp.bfloat16)
            a_ref[g, :, :eofs] = high
            a_ref[g, :, lanes : lanes + eofs] = low


def fold(requests, slots, counts, weights, eofs, src_tiles):
    grids, tile_total, pairs, cells, cells_x = weights.shape
    cap = requests.shape[1] // 2
    lanes = pl.cdiv(eofs.shape[0], 128) * 128
    tiles = 4
    weights = stay(weights.reshape(grids, tile_total, pairs * cells, cells_x))
    flops = 2 * grids * tile_total * pairs * cells * cells_x * eofs.shape[0]
    return pl.pallas_call(
        functools.partial(fold_kernel, src_tiles),
        out_shape=jax.ShapeDtypeStruct((grids, 3 * cap * cells, 2 * lanes), jnp.bfloat16),
        grid=(tile_total // tiles,),
        in_specs=[
            SMEM,
            SMEM,
            SMEM,
            pl.BlockSpec((grids, tiles, pairs * cells, cells_x), lambda i: (0, i, 0, 0)),
            pl.BlockSpec((eofs.shape[0], tiles * cells_x), lambda i: (0, i)),
        ],
        out_specs=pl.BlockSpec((grids, 3 * cap * cells, 2 * lanes), lambda i: (0, 0, 0)),
        scratch_shapes=[pltpu.SMEM((grids, 2 * cap), jnp.int32)]
        + [pltpu.VMEM(((3 * cap + 1) * cells, eofs.shape[0]), jnp.float32)] * grids,
        cost_estimate=pl.CostEstimate(
            flops=8 * flops, bytes_accessed=weights.size * 2, transcendentals=0
        ),
        compiler_params=grant(20),
        name="fold",
    )(requests, slots, counts, weights, eofs)


def times(source, folded):
    return lax.dot_general(
        source, folded, (((0,), (0,)), ((), ())), preferred_element_type=jnp.float32
    )


def near_kernel(requests, fields, others, a_ref, near_ref, order, chosen):
    lat, lon, pair, cross, base, lon_count = place()
    grids, src_tiles, cells, columns = fields.shape
    cap = order.shape[0] - 1
    eofs = near_ref.shape[1]
    lanes = a_ref.shape[2] // 2
    for g in range(grids):
        for k, (owner, source) in enumerate(((lon, fields), (pair, others))):
            list_tiles(requests, order, g, base + lon, base + owner, src_tiles)
            for j in range(cap):
                row = (k * cap + j) * cells
                chosen[row : row + cells, :] = source[g, order[j]]
        total = times(chosen[...], a_ref[g, : 2 * cap * cells, :])
        near_ref[g * columns : (g + 1) * columns, :] = (
            total[:, :eofs] + total[:, lanes : lanes + eofs]
        )


def near(requests, fields, others, folded, eofs):
    grids, src_tiles, cells, columns = fields.shape
    cap = requests.shape[1] // 2
    return pl.pallas_call(
        near_kernel,
        out_shape=jax.ShapeDtypeStruct((grids * columns, eofs), jnp.float32),
        in_specs=[SMEM, VMEM, VMEM, VMEM],
        out_specs=VMEM,
        scratch_shapes=[
            pltpu.SMEM((cap + 1,), jnp.int32),
            pltpu.VMEM((2 * cap * cells, columns), fields.dtype),
        ],
        cost_estimate=pl.CostEstimate(flops=10**9, bytes_accessed=10**6, transcendentals=0),
        compiler_params=grant(12),
        name="near",
    )(requests, fields, others, folded)


def far_kernel(lat_count, near_ref, tiles, a_ref, keep_ref, send_ref, whole, units):
    lat, lon, pair, cross, base, lon_count = place()
    grids, cap, cells, columns = tiles.shape
    eofs = near_ref.shape[1]
    lanes = a_ref.shape[2] // 2
    planes = lon_count // CORES
    rows = units.shape[1]
    for g in range(grids):
        part = slice(g * columns, (g + 1) * columns)
        total = times(tiles[g].reshape(cap * cells, columns), a_ref[g, 2 * cap * cells :, :])
        product = near_ref[part, :] + total[:, :eofs] + total[:, lanes : lanes + eofs]
        product = product.reshape(columns // MONTHS, MONTHS, eofs)
        product = product - jnp.mean(product, axis=1, keepdims=True)
        whole[part, :] = product.reshape(columns, eofs)
    for u in range(units.shape[0]):
        units[u] = whole[u * rows : (u + 1) * rows, :]
    plane, core = lax.div(lon, CORES), lax.rem(lon, CORES)
    for c, out in ((0, keep_ref), (1, send_ref)):
        for r in range(planes):
            for q in range(lat_count):
                target = jnp.bitwise_xor(lat, q) * lon_count
                target += jnp.bitwise_xor(plane, r) * CORES + jnp.bitwise_xor(core, c)
                out[r, q * rows : (q + 1) * rows, :] = units[target]


def far(near_part, tiles, folded):
    lat_count, lon_count = lax.axis_size("lat"), lax.axis_size("lon")
    total_columns, eofs = near_part.shape
    rows = total_columns // (lat_count * lon_count)
    block = jax.ShapeDtypeStruct((lon_count // CORES, lat_count * rows, eofs), jnp.float32)
    return pl.pallas_call(
        functools.partial(far_kernel, lat_count),
        out_shape=(block, block),
        in_specs=[VMEM, VMEM, VMEM],
        out_specs=(VMEM, VMEM),
        scratch_shapes=[
            pltpu.VMEM((total_columns, eofs), jnp.float32),
            pltpu.VMEM((lat_count * lon_count, rows, eofs), jnp.float32),
        ],
        compiler_params=grant(16),
        name="far",
    )(near_part, tiles, folded)


def shards(fields, weights, pair_slots, pair_counts, requests, eofs):
    lat_count, lon_count = lax.axis_size("lat"), lax.axis_size("lon")
    planes = lon_count // CORES
    requests = stay(requests.transpose(0, 2, 1))
    pair_slots = stay(pair_slots.transpose(0, 2, 1))
    pair_counts = stay(pair_counts)
    eofs = stay(eofs)
    on_chip = [(i, i ^ 1) for i in range(lon_count)]
    off_chip = [(i, (i + 2 * (i % CORES) - 1) % lon_count) for i in range(lon_count)]
    tiles = lax.ppermute(pick(requests, stay(fields)), "lon", off_chip)
    others = lax.ppermute(fields, "lon", on_chip)
    folded = fold(requests, pair_slots, pair_counts, weights, eofs, fields.shape[1])
    near_part = near(requests, fields, others, folded, eofs.shape[0])
    keep, send = far(near_part, tiles, folded)
    pair_sum = keep + lax.ppermute(send, "lon", on_chip)
    plane_sum = pair_sum[0]
    for r in range(1, planes):
        swap = [(i, i ^ (r * CORES)) for i in range(lon_count)]
        sent = lax.ppermute(pair_sum[r].astype(jnp.bfloat16), "lon", swap)
        plane_sum = plane_sum + sent.astype(jnp.float32)
    rows = plane_sum.shape[0] // lat_count
    total = plane_sum[:rows]
    for q in range(1, lat_count):
        swap = [(i, i ^ q) for i in range(lat_count)]
        total = total + lax.ppermute(plane_sum[q * rows : (q + 1) * rows], "lat", swap)
    return total.T


def solution(mesh):
    return jax.shard_map(
        shards,
        mesh=mesh,
        in_specs=(
            P(None, ("lat", "lon"), None, None),
            P(None, ("lat", "lon"), None, None, None),
            P(None, ("lat", "lon"), None),
            P(None, ("lat", "lon")),
            P(),
            P(None, ("lat", "lon")),
        ),
        out_specs=P(None, ("lat", "lon")),
        check_vma=False,
    )
```

```python
import functools

import jax
import jax.numpy as jnp
from jax import lax
from jax.experimental import pallas as pl
from jax.experimental.pallas import tpu as pltpu
from jax.sharding import PartitionSpec as P


MONTHS = 24
CORES = 2
MIB = 2**20

SMEM = pl.BlockSpec(memory_space=pltpu.SMEM)
VMEM = pl.BlockSpec(memory_space=pltpu.VMEM)
HBM = pl.BlockSpec(memory_space=pl.ANY)


def grant(size):
    return pltpu.CompilerParams(vmem_limit_bytes=size * MIB)


def stay(array):
    return pltpu.with_memory_space_constraint(array, pltpu.HBM)


def place():
    lat, lon, lon_count = lax.axis_index("lat"), lax.axis_index("lon"), lax.axis_size("lon")
    core = lax.rem(lon, CORES)
    pair = lon + 1 - 2 * core
    cross = lax.rem(lon + 2 * core - 1 + lon_count, lon_count)
    return lat, lon, pair, cross, lat * lon_count, lon_count


def list_tiles(requests, order, g, reader, owner, src_tiles):
    rank = jnp.int32(0)
    for r in range(requests.shape[1]):
        local = requests[g, r, reader] - owner * src_tiles
        hit = jnp.logical_and(local >= 0, local < src_tiles)
        order[rank] = jnp.where(hit, local, 0)
        rank += hit.astype(jnp.int32)
    return [jnp.where(j < rank, order[j], 0) for j in range(order.shape[0] - 1)]


def pick_kernel(requests_ref, fields_ref, out_ref, requests, fields, sems, *orders):
    _, lon, _, cross, base, _ = place()
    grids, src_tiles = fields.shape[:2]
    listing = pltpu.make_async_copy(requests_ref, requests, sems.at[grids])
    listing.start()
    loads = [pltpu.make_async_copy(fields_ref.at[g], fields.at[g], sems.at[g]) for g in range(grids)]
    for load in loads:
        load.start()
    listing.wait()
    listed = [
        list_tiles(requests, orders[g], g, base + cross, base + lon, src_tiles) for g in range(grids)
    ]
    for g in range(grids):
        loads[g].wait()
        for j, tile in enumerate(listed[g]):
            out_ref[g, j] = fields[g, tile]


def pick(requests, fields):
    grids, _, cells, columns = fields.shape
    cap = requests.shape[1] // 2
    return pl.pallas_call(
        pick_kernel,
        out_shape=jax.ShapeDtypeStruct((grids, cap, cells, columns), fields.dtype),
        in_specs=[HBM, HBM],
        out_specs=VMEM,
        scratch_shapes=[
            pltpu.SMEM(requests.shape, jnp.int32),
            pltpu.VMEM(fields.shape, fields.dtype),
            pltpu.SemaphoreType.DMA((grids + 1,)),
        ]
        + [pltpu.SMEM((cap + 1,), jnp.int32)] * grids,
        compiler_params=grant(6),
        name="pick",
    )(requests, fields)


def fold_kernel(src_tiles, requests, slots_ref, counts_ref, w_ref, e_ref, a_ref, where, *totals):
    step = pl.program_id(0)
    grids, tiles, depth, cells_x = w_ref.shape
    slots = requests.shape[1]
    cap = slots // 2
    pairs = slots_ref.shape[1]
    cells = depth // pairs
    eofs = e_ref.shape[0]
    lanes = a_ref.shape[2] // 2
    _, lon, pair, _, base, _ = place()

    @pl.when(step == 0)
    def _():
        for total in totals:
            total[...] = jnp.zeros_like(total)
        for g in range(grids):
            ranks = [jnp.int32(0)] * 3
            for r in range(slots):
                owner = lax.div(requests[g, r, base + lon], src_tiles) - base
                hits = [(owner == k).astype(jnp.int32) for k in (lon, pair)]
                hits.append(1 - hits[0] - hits[1])
                where[g, r] = sum(h * (k * cap + n) for k, (h, n) in enumerate(zip(hits, ranks)))
                ranks = [n + h for n, h in zip(ranks, hits)]

    for t in range(tiles):
        tile = step * tiles + t
        basis = e_ref[:, t * cells_x : (t + 1) * cells_x]
        parts = [
            lax.dot_general(
                w_ref[g, t], basis, (((1,), (1,)), ((), ())), preferred_element_type=jnp.float32
            )
            for g in range(grids)
        ]
        for p in range(pairs):
            for g in range(grids):
                spot = where[g, slots_ref[g, p, tile]]
                spot = jnp.where(p < counts_ref[g, tile], spot, 3 * cap)
                rows = pl.ds(pl.multiple_of(spot * cells, cells), cells)
                totals[g][rows, :] += parts[g][p * cells : (p + 1) * cells]

    @pl.when(step == pl.num_programs(0) - 1)
    def _():
        for g in range(grids):
            total = totals[g][: 3 * cap * cells, :]
            high = total.astype(jnp.bfloat16)
            low = (total - high.astype(jnp.float32)).astype(jnp.bfloat16)
            a_ref[g, :, :eofs] = high
            a_ref[g, :, lanes : lanes + eofs] = low


def fold(requests, slots, counts, weights, eofs, src_tiles):
    grids, tile_total, pairs, cells, cells_x = weights.shape
    cap = requests.shape[1] // 2
    lanes = pl.cdiv(eofs.shape[0], 128) * 128
    tiles = 4
    weights = stay(weights.reshape(grids, tile_total, pairs * cells, cells_x))
    flops = 2 * grids * tile_total * pairs * cells * cells_x * eofs.shape[0]
    return pl.pallas_call(
        functools.partial(fold_kernel, src_tiles),
        out_shape=jax.ShapeDtypeStruct((grids, 3 * cap * cells, 2 * lanes), jnp.bfloat16),
        grid=(tile_total // tiles,),
        in_specs=[
            SMEM,
            SMEM,
            SMEM,
            pl.BlockSpec((grids, tiles, pairs * cells, cells_x), lambda i: (0, i, 0, 0)),
            pl.BlockSpec((eofs.shape[0], tiles * cells_x), lambda i: (0, i)),
        ],
        out_specs=pl.BlockSpec((grids, 3 * cap * cells, 2 * lanes), lambda i: (0, 0, 0)),
        scratch_shapes=[pltpu.SMEM((grids, 2 * cap), jnp.int32)]
        + [pltpu.VMEM(((3 * cap + 1) * cells, eofs.shape[0]), jnp.float32)] * grids,
        cost_estimate=pl.CostEstimate(
            flops=8 * flops, bytes_accessed=weights.size * 2, transcendentals=0
        ),
        compiler_params=grant(20),
        name="fold",
    )(requests, slots, counts, weights, eofs)


def times(source, folded):
    return lax.dot_general(
        source, folded, (((0,), (0,)), ((), ())), preferred_element_type=jnp.float32
    )


def near_kernel(requests, fields, others, a_ref, near_ref, order, chosen):
    _, lon, pair, _, base, _ = place()
    grids, src_tiles, cells, columns = fields.shape
    cap = order.shape[0] - 1
    eofs = near_ref.shape[1]
    lanes = a_ref.shape[2] // 2
    for g in range(grids):
        for k, (owner, source) in enumerate(((lon, fields), (pair, others))):
            listed = list_tiles(requests, order, g, base + lon, base + owner, src_tiles)
            for j in range(cap):
                row = (k * cap + j) * cells
                chosen[row : row + cells, :] = source[g, listed[j]]
        total = times(chosen[...], a_ref[g, : 2 * cap * cells, :])
        near_ref[g * columns : (g + 1) * columns, :] = (
            total[:, :eofs] + total[:, lanes : lanes + eofs]
        )


def near(requests, fields, others, folded, eofs):
    grids, _, cells, columns = fields.shape
    cap = requests.shape[1] // 2
    return pl.pallas_call(
        near_kernel,
        out_shape=jax.ShapeDtypeStruct((grids * columns, eofs), jnp.float32),
        in_specs=[SMEM, VMEM, VMEM, VMEM],
        out_specs=VMEM,
        scratch_shapes=[
            pltpu.SMEM((cap + 1,), jnp.int32),
            pltpu.VMEM((2 * cap * cells, columns), fields.dtype),
        ],
        cost_estimate=pl.CostEstimate(flops=10**9, bytes_accessed=10**6, transcendentals=0),
        compiler_params=grant(12),
        name="near",
    )(requests, fields, others, folded)


def far_kernel(lat_count, near_ref, tiles, a_ref, keep_ref, send_ref, whole, units):
    lat, lon, _, _, _, lon_count = place()
    grids, cap, cells, columns = tiles.shape
    eofs = near_ref.shape[1]
    lanes = a_ref.shape[2] // 2
    planes = lon_count // CORES
    rows = units.shape[1]
    for g in range(grids):
        part = slice(g * columns, (g + 1) * columns)
        total = times(tiles[g].reshape(cap * cells, columns), a_ref[g, 2 * cap * cells :, :])
        product = near_ref[part, :] + total[:, :eofs] + total[:, lanes : lanes + eofs]
        product = product.reshape(columns // MONTHS, MONTHS, eofs)
        product = product - jnp.mean(product, axis=1, keepdims=True)
        whole[part, :] = product.reshape(columns, eofs)
    for u in range(units.shape[0]):
        units[u] = whole[u * rows : (u + 1) * rows, :]
    plane, core = lax.div(lon, CORES), lax.rem(lon, CORES)
    for c, out in ((0, keep_ref), (1, send_ref)):
        for r in range(planes):
            for q in range(lat_count):
                target = jnp.bitwise_xor(lat, q) * lon_count
                target += jnp.bitwise_xor(plane, r) * CORES + jnp.bitwise_xor(core, c)
                out[r, q * rows : (q + 1) * rows, :] = units[target]


def far(near_part, tiles, folded):
    lat_count, lon_count = lax.axis_size("lat"), lax.axis_size("lon")
    total_columns, eofs = near_part.shape
    rows = total_columns // (lat_count * lon_count)
    block = jax.ShapeDtypeStruct((lon_count // CORES, lat_count * rows, eofs), jnp.float32)
    return pl.pallas_call(
        functools.partial(far_kernel, lat_count),
        out_shape=(block, block),
        in_specs=[VMEM, VMEM, VMEM],
        out_specs=(VMEM, VMEM),
        scratch_shapes=[
            pltpu.VMEM((total_columns, eofs), jnp.float32),
            pltpu.VMEM((lat_count * lon_count, rows, eofs), jnp.float32),
        ],
        compiler_params=grant(16),
        name="far",
    )(near_part, tiles, folded)


def shards(fields, weights, pair_slots, pair_counts, requests, eofs):
    lat_count, lon_count = lax.axis_size("lat"), lax.axis_size("lon")
    planes = lon_count // CORES
    requests = stay(requests.transpose(0, 2, 1))
    pair_slots = stay(pair_slots.transpose(0, 2, 1))
    pair_counts = stay(pair_counts)
    eofs = stay(eofs)
    on_chip = [(i, i ^ 1) for i in range(lon_count)]
    off_chip = [(i, (i + 2 * (i % CORES) - 1) % lon_count) for i in range(lon_count)]
    picked, later = lax.optimization_barrier((pick(requests, stay(fields)), fields))
    tiles = lax.ppermute(picked, "lon", off_chip)
    others = lax.ppermute(later, "lon", on_chip)
    folded = fold(requests, pair_slots, pair_counts, weights, eofs, fields.shape[1])
    near_part = near(requests, fields, others, folded, eofs.shape[0])
    keep, send = far(near_part, tiles, folded)
    pair_sum = keep + lax.ppermute(send, "lon", on_chip)
    plane_sum = pair_sum[0]
    for r in reversed(range(1, planes)):
        swap = [(i, i ^ (r * CORES)) for i in range(lon_count)]
        sent = lax.ppermute(pair_sum[r].astype(jnp.bfloat16), "lon", swap)
        plane_sum = plane_sum + sent.astype(jnp.float32)
    rows = plane_sum.shape[0] // lat_count
    total = plane_sum[:rows]
    for q in reversed(range(1, lat_count)):
        swap = [(i, i ^ q) for i in range(lat_count)]
        total = total + lax.ppermute(plane_sum[q * rows : (q + 1) * rows], "lat", swap)
    return total.T


def solution(mesh):
    return jax.shard_map(
        shards,
        mesh=mesh,
        in_specs=(
            P(None, ("lat", "lon"), None, None),
            P(None, ("lat", "lon"), None, None, None),
            P(None, ("lat", "lon"), None),
            P(None, ("lat", "lon")),
            P(),
            P(None, ("lat", "lon")),
        ),
        out_specs=P(None, ("lat", "lon")),
        check_vma=False,
    )
```

```python
import functools

import jax
import jax.numpy as jnp
from jax import lax
from jax.experimental import pallas as pl
from jax.experimental.pallas import tpu as pltpu
from jax.sharding import PartitionSpec as P


MONTHS = 24
CORES = 2
MIB = 2**20

SMEM = pl.BlockSpec(memory_space=pltpu.SMEM)
VMEM = pl.BlockSpec(memory_space=pltpu.VMEM)
HBM = pl.BlockSpec(memory_space=pl.ANY)


def grant(size):
    return pltpu.CompilerParams(vmem_limit_bytes=size * MIB)


def stay(array):
    return pltpu.with_memory_space_constraint(array, pltpu.HBM)


def place():
    lat, lon, lon_count = lax.axis_index("lat"), lax.axis_index("lon"), lax.axis_size("lon")
    core = lax.rem(lon, CORES)
    pair = lon + 1 - 2 * core
    cross = lax.rem(lon + 2 * core - 1 + lon_count, lon_count)
    return lat, lon, pair, cross, lat * lon_count, lon_count


def list_tiles(requests, order, g, reader, owner, src_tiles):
    rank = jnp.int32(0)
    for r in range(requests.shape[1]):
        local = requests[g, r, reader] - owner * src_tiles
        hit = jnp.logical_and(local >= 0, local < src_tiles)
        order[rank] = jnp.where(hit, local, 0)
        rank += hit.astype(jnp.int32)
    return [jnp.where(j < rank, order[j], 0) for j in range(order.shape[0] - 1)]


def pick_kernel(requests_ref, fields_ref, sent_ref, kept_ref, requests, fields, sems, *orders):
    _, lon, _, cross, base, _ = place()
    grids, src_tiles = fields.shape[:2]
    listing = pltpu.make_async_copy(requests_ref, requests, sems.at[grids])
    listing.start()
    loads = [pltpu.make_async_copy(fields_ref.at[g], fields.at[g], sems.at[g]) for g in range(grids)]
    for load in loads:
        load.start()
    listing.wait()
    listed = [
        list_tiles(requests, orders[g], g, base + cross, base + lon, src_tiles) for g in range(grids)
    ]
    for g in range(grids):
        loads[g].wait()
        for j, tile in enumerate(listed[g]):
            if g < grids - 1:
                sent_ref[g, j] = fields[g, tile]
            else:
                kept_ref[j] = fields[g, tile]


def pick(requests, fields):
    grids, _, cells, columns = fields.shape
    cap = requests.shape[1] // 2
    return pl.pallas_call(
        pick_kernel,
        out_shape=(
            jax.ShapeDtypeStruct((grids - 1, cap, cells, columns), fields.dtype),
            jax.ShapeDtypeStruct((cap, cells, columns), fields.dtype),
        ),
        in_specs=[HBM, HBM],
        out_specs=(VMEM, VMEM),
        scratch_shapes=[
            pltpu.SMEM(requests.shape, jnp.int32),
            pltpu.VMEM(fields.shape, fields.dtype),
            pltpu.SemaphoreType.DMA((grids + 1,)),
        ]
        + [pltpu.SMEM((cap + 1,), jnp.int32)] * grids,
        compiler_params=grant(6),
        name="pick",
    )(requests, fields)


def fold_kernel(
    src_tiles, requests, slots_ref, counts_ref, w_ref, e_ref, a_ref, sent_ref, where, *totals
):
    step = pl.program_id(0)
    grids, tiles, depth, cells_x = w_ref.shape
    slots = requests.shape[1]
    cap = slots // 2
    pairs = slots_ref.shape[1]
    cells = depth // pairs
    eofs = e_ref.shape[0]
    lanes = a_ref.shape[2] // 2
    _, lon, pair, _, base, _ = place()

    @pl.when(step == 0)
    def _():
        for total in totals:
            total[...] = jnp.zeros_like(total)
        for g in range(grids):
            ranks = [jnp.int32(0)] * 3
            for r in range(slots):
                owner = lax.div(requests[g, r, base + lon], src_tiles) - base
                hits = [(owner == k).astype(jnp.int32) for k in (lon, pair)]
                hits.append(1 - hits[0] - hits[1])
                where[g, r] = sum(h * (k * cap + n) for k, (h, n) in enumerate(zip(hits, ranks)))
                ranks = [n + h for n, h in zip(ranks, hits)]

    for t in range(tiles):
        tile = step * tiles + t
        basis = e_ref[:, t * cells_x : (t + 1) * cells_x]
        parts = [
            lax.dot_general(
                w_ref[g, t], basis, (((1,), (1,)), ((), ())), preferred_element_type=jnp.float32
            )
            for g in range(grids)
        ]
        for p in range(pairs):
            for g in range(grids):
                spot = where[g, slots_ref[g, p, tile]]
                spot = jnp.where(p < counts_ref[g, tile], spot, 3 * cap)
                rows = pl.ds(pl.multiple_of(spot * cells, cells), cells)
                totals[g][rows, :] += parts[g][p * cells : (p + 1) * cells]

    @pl.when(step == pl.num_programs(0) - 1)
    def _():
        for g in range(grids):
            total = totals[g][: 3 * cap * cells, :]
            high = total.astype(jnp.bfloat16)
            low = (total - high.astype(jnp.float32)).astype(jnp.bfloat16)
            a_ref[g, :, :eofs] = high
            a_ref[g, :, lanes : lanes + eofs] = low
            if g == grids - 1:
                sent_ref[...] = high[2 * cap * cells :, :]


def fold(requests, slots, counts, weights, eofs, src_tiles):
    grids, tile_total, pairs, cells, cells_x = weights.shape
    cap = requests.shape[1] // 2
    lanes = pl.cdiv(eofs.shape[0], 128) * 128
    tiles = tile_total // 2
    weights = stay(weights.reshape(grids, tile_total, pairs * cells, cells_x))
    flops = 2 * grids * tile_total * pairs * cells * cells_x * eofs.shape[0]
    return pl.pallas_call(
        functools.partial(fold_kernel, src_tiles),
        out_shape=(
            jax.ShapeDtypeStruct((grids, 3 * cap * cells, 2 * lanes), jnp.bfloat16),
            jax.ShapeDtypeStruct((cap * cells, eofs.shape[0]), jnp.bfloat16),
        ),
        grid=(tile_total // tiles,),
        in_specs=[
            SMEM,
            SMEM,
            SMEM,
            pl.BlockSpec((grids, tiles, pairs * cells, cells_x), lambda i: (0, i, 0, 0)),
            pl.BlockSpec((eofs.shape[0], tiles * cells_x), lambda i: (0, i)),
        ],
        out_specs=(
            pl.BlockSpec((grids, 3 * cap * cells, 2 * lanes), lambda i: (0, 0, 0)),
            pl.BlockSpec((cap * cells, eofs.shape[0]), lambda i: (0, 0)),
        ),
        scratch_shapes=[pltpu.SMEM((grids, 2 * cap), jnp.int32)]
        + [pltpu.VMEM(((3 * cap + 1) * cells, eofs.shape[0]), jnp.float32)] * grids,
        cost_estimate=pl.CostEstimate(
            flops=8 * flops, bytes_accessed=weights.size * 2, transcendentals=0
        ),
        compiler_params=grant(20),
        name="fold",
    )(requests, slots, counts, weights, eofs)


def times(source, folded):
    return lax.dot_general(
        source, folded, (((0,), (0,)), ((), ())), preferred_element_type=jnp.float32
    )


def near_kernel(requests, fields, others, a_ref, near_ref, order, chosen):
    _, lon, pair, _, base, _ = place()
    grids, src_tiles, cells, columns = fields.shape
    cap = order.shape[0] - 1
    eofs = near_ref.shape[1]
    lanes = a_ref.shape[2] // 2
    for g in range(grids):
        for k, (owner, source) in enumerate(((lon, fields), (pair, others))):
            listed = list_tiles(requests, order, g, base + lon, base + owner, src_tiles)
            for j in range(cap):
                row = (k * cap + j) * cells
                chosen[row : row + cells, :] = source[g, listed[j]]
        total = times(chosen[...], a_ref[g, : 2 * cap * cells, :])
        near_ref[g * columns : (g + 1) * columns, :] = (
            total[:, :eofs] + total[:, lanes : lanes + eofs]
        )


def near(requests, fields, others, folded, eofs):
    grids, _, cells, columns = fields.shape
    cap = requests.shape[1] // 2
    return pl.pallas_call(
        near_kernel,
        out_shape=jax.ShapeDtypeStruct((grids * columns, eofs), jnp.float32),
        in_specs=[SMEM, VMEM, VMEM, VMEM],
        out_specs=VMEM,
        scratch_shapes=[
            pltpu.SMEM((cap + 1,), jnp.int32),
            pltpu.VMEM((2 * cap * cells, columns), fields.dtype),
        ],
        cost_estimate=pl.CostEstimate(flops=10**9, bytes_accessed=10**6, transcendentals=0),
        compiler_params=grant(12),
        name="near",
    )(requests, fields, others, folded)


def far_kernel(lat_count, near_ref, tiles, kept, a_ref, others_ref, keep_ref, send_ref, whole, units):
    lat, lon, _, _, _, lon_count = place()
    grids, cap, cells, columns = tiles.shape[0] + 1, *tiles.shape[1:]
    eofs = near_ref.shape[1]
    lanes = a_ref.shape[2] // 2
    planes = lon_count // CORES
    rows = units.shape[1]
    for g in range(grids):
        part = slice(g * columns, (g + 1) * columns)
        if g < grids - 1:
            total = times(tiles[g].reshape(cap * cells, columns), a_ref[g, 2 * cap * cells :, :])
            total = total[:, :eofs] + total[:, lanes : lanes + eofs]
        else:
            total = times(kept[...].reshape(cap * cells, columns), others_ref[...])
        product = near_ref[part, :] + total
        product = product.reshape(columns // MONTHS, MONTHS, eofs)
        product = product - jnp.mean(product, axis=1, keepdims=True)
        whole[part, :] = product.reshape(columns, eofs)
    for u in range(units.shape[0]):
        units[u] = whole[u * rows : (u + 1) * rows, :]
    plane, core = lax.div(lon, CORES), lax.rem(lon, CORES)
    for c, out in ((0, keep_ref), (1, send_ref)):
        for r in range(planes):
            for q in range(lat_count):
                target = jnp.bitwise_xor(lat, q) * lon_count
                target += jnp.bitwise_xor(plane, r) * CORES + jnp.bitwise_xor(core, c)
                out[r, q * rows : (q + 1) * rows, :] = units[target]


def far(near_part, tiles, kept, folded, others):
    lat_count, lon_count = lax.axis_size("lat"), lax.axis_size("lon")
    total_columns, eofs = near_part.shape
    rows = total_columns // (lat_count * lon_count)
    block = jax.ShapeDtypeStruct((lon_count // CORES, lat_count * rows, eofs), jnp.float32)
    return pl.pallas_call(
        functools.partial(far_kernel, lat_count),
        out_shape=(block, block),
        in_specs=[VMEM] * 5,
        out_specs=(VMEM, VMEM),
        scratch_shapes=[
            pltpu.VMEM((total_columns, eofs), jnp.float32),
            pltpu.VMEM((lat_count * lon_count, rows, eofs), jnp.float32),
        ],
        compiler_params=grant(16),
        name="far",
    )(near_part, tiles, kept, folded, others)


def shards(fields, weights, pair_slots, pair_counts, requests, eofs):
    lat_count, lon_count = lax.axis_size("lat"), lax.axis_size("lon")
    planes = lon_count // CORES
    requests = stay(requests.transpose(0, 2, 1))
    pair_slots = stay(pair_slots.transpose(0, 2, 1))
    pair_counts = stay(pair_counts)
    eofs = stay(eofs)
    on_chip = [(i, i ^ 1) for i in range(lon_count)]
    off_chip = [(i, (i + 2 * (i % CORES) - 1) % lon_count) for i in range(lon_count)]
    (picked, kept), later = lax.optimization_barrier((pick(requests, stay(fields)), fields))
    tiles = lax.ppermute(picked, "lon", off_chip)
    others = lax.ppermute(later, "lon", on_chip)
    folded, spread = fold(requests, pair_slots, pair_counts, weights, eofs, fields.shape[1])
    spread = lax.ppermute(spread, "lon", off_chip)
    near_part = near(requests, fields, others, folded, eofs.shape[0])
    keep, send = far(near_part, tiles, kept, folded, spread)
    pair_sum = keep + lax.ppermute(send, "lon", on_chip)
    plane_sum = pair_sum[0]
    for r in reversed(range(1, planes)):
        swap = [(i, i ^ (r * CORES)) for i in range(lon_count)]
        sent = lax.ppermute(pair_sum[r].astype(jnp.bfloat16), "lon", swap)
        plane_sum = plane_sum + sent.astype(jnp.float32)
    rows = plane_sum.shape[0] // lat_count
    total = plane_sum[:rows]
    for q in reversed(range(1, lat_count)):
        swap = [(i, i ^ q) for i in range(lat_count)]
        total = total + lax.ppermute(plane_sum[q * rows : (q + 1) * rows], "lat", swap)
    return total.T


def solution(mesh):
    return jax.shard_map(
        shards,
        mesh=mesh,
        in_specs=(
            P(None, ("lat", "lon"), None, None),
            P(None, ("lat", "lon"), None, None, None),
            P(None, ("lat", "lon"), None),
            P(None, ("lat", "lon")),
            P(),
            P(None, ("lat", "lon")),
        ),
        out_specs=P(None, ("lat", "lon")),
        check_vma=False,
    )
```

```python
import functools

import jax
import jax.numpy as jnp
from jax import lax
from jax.experimental import pallas as pl
from jax.experimental.pallas import tpu as pltpu
from jax.sharding import PartitionSpec as P


MONTHS = 24
CORES = 2
MIB = 2**20

SMEM = pl.BlockSpec(memory_space=pltpu.SMEM)
VMEM = pl.BlockSpec(memory_space=pltpu.VMEM)
HBM = pl.BlockSpec(memory_space=pl.ANY)


def grant(size):
    return pltpu.CompilerParams(vmem_limit_bytes=size * MIB)


def stay(array):
    return pltpu.with_memory_space_constraint(array, pltpu.HBM)


def place():
    lat, lon, lon_count = lax.axis_index("lat"), lax.axis_index("lon"), lax.axis_size("lon")
    core = lax.rem(lon, CORES)
    pair = lon + 1 - 2 * core
    cross = lax.rem(lon + 2 * core - 1 + lon_count, lon_count)
    return lat, lon, pair, cross, lat * lon_count, lon_count


def list_tiles(requests, order, g, reader, owner, src_tiles):
    rank = jnp.int32(0)
    for r in range(requests.shape[1]):
        local = requests[g, r, reader] - owner * src_tiles
        hit = jnp.logical_and(local >= 0, local < src_tiles)
        order[rank] = jnp.where(hit, local, 0)
        rank += hit.astype(jnp.int32)
    return [jnp.where(j < rank, order[j], 0) for j in range(order.shape[0] - 1)]


def pick_kernel(requests_ref, fields_ref, sent_ref, requests, fields, sems, *orders):
    _, lon, _, cross, base, _ = place()
    grids, src_tiles = fields.shape[:2]
    listing = pltpu.make_async_copy(requests_ref.at[:grids], requests, sems.at[grids])
    listing.start()
    loads = [pltpu.make_async_copy(fields_ref.at[g], fields.at[g], sems.at[g]) for g in range(grids)]
    for load in loads:
        load.start()
    listing.wait()
    listed = [
        list_tiles(requests, orders[g], g, base + cross, base + lon, src_tiles) for g in range(grids)
    ]
    for g in range(grids):
        loads[g].wait()
        for j, tile in enumerate(listed[g]):
            sent_ref[g, j] = fields[g, tile]


def pick(requests, fields):
    grids, src_tiles, cells, columns = fields.shape
    grids -= 1
    cap = requests.shape[1] // 2
    return pl.pallas_call(
        pick_kernel,
        out_shape=jax.ShapeDtypeStruct((grids, cap, cells, columns), fields.dtype),
        in_specs=[HBM, HBM],
        out_specs=VMEM,
        scratch_shapes=[
            pltpu.SMEM((grids, *requests.shape[1:]), jnp.int32),
            pltpu.VMEM((grids, src_tiles, cells, columns), fields.dtype),
            pltpu.SemaphoreType.DMA((grids + 1,)),
        ]
        + [pltpu.SMEM((cap + 1,), jnp.int32)] * grids,
        compiler_params=grant(6),
        name="pick",
    )(requests, fields)


def fold_kernel(
    src_tiles, requests, slots_ref, counts_ref, w_ref, e_ref, a_ref, sent_ref, where, *totals
):
    step = pl.program_id(0)
    grids, tiles, depth, cells_x = w_ref.shape
    slots = requests.shape[1]
    cap = slots // 2
    pairs = slots_ref.shape[1]
    cells = depth // pairs
    eofs = e_ref.shape[0]
    lanes = a_ref.shape[2] // 2
    _, lon, pair, _, base, _ = place()

    @pl.when(step == 0)
    def _():
        for total in totals:
            total[...] = jnp.zeros_like(total)
        for g in range(grids):
            ranks = [jnp.int32(0)] * 3
            for r in range(slots):
                owner = lax.div(requests[g, r, base + lon], src_tiles) - base
                hits = [(owner == k).astype(jnp.int32) for k in (lon, pair)]
                hits.append(1 - hits[0] - hits[1])
                where[g, r] = sum(h * (k * cap + n) for k, (h, n) in enumerate(zip(hits, ranks)))
                ranks = [n + h for n, h in zip(ranks, hits)]

    for t in range(tiles):
        tile = step * tiles + t
        basis = e_ref[:, t * cells_x : (t + 1) * cells_x]
        parts = [
            lax.dot_general(
                w_ref[g, t], basis, (((1,), (1,)), ((), ())), preferred_element_type=jnp.float32
            )
            for g in range(grids)
        ]
        for p in range(pairs):
            for g in range(grids):
                spot = where[g, slots_ref[g, p, tile]]
                spot = jnp.where(p < counts_ref[g, tile], spot, 3 * cap)
                rows = pl.ds(pl.multiple_of(spot * cells, cells), cells)
                totals[g][rows, :] += parts[g][p * cells : (p + 1) * cells]

    @pl.when(step == pl.num_programs(0) - 1)
    def _():
        for g in range(grids):
            total = totals[g][: 3 * cap * cells, :]
            high = total.astype(jnp.bfloat16)
            low = (total - high.astype(jnp.float32)).astype(jnp.bfloat16)
            a_ref[g, :, :eofs] = high
            a_ref[g, :, lanes : lanes + eofs] = low
            if g == grids - 1:
                for j in range(cap):
                    row = (2 * cap + j) * cells
                    sent_ref[:, j * eofs : (j + 1) * eofs] = high[row : row + cells, :]


def fold(requests, slots, counts, weights, eofs, src_tiles):
    grids, tile_total, pairs, cells, cells_x = weights.shape
    cap = requests.shape[1] // 2
    lanes = pl.cdiv(eofs.shape[0], 128) * 128
    tiles = tile_total // 2
    weights = stay(weights.reshape(grids, tile_total, pairs * cells, cells_x))
    flops = 2 * grids * tile_total * pairs * cells * cells_x * eofs.shape[0]
    return pl.pallas_call(
        functools.partial(fold_kernel, src_tiles),
        out_shape=(
            jax.ShapeDtypeStruct((grids, 3 * cap * cells, 2 * lanes), jnp.bfloat16),
            jax.ShapeDtypeStruct((cells, cap * eofs.shape[0]), jnp.bfloat16),
        ),
        grid=(tile_total // tiles,),
        in_specs=[
            SMEM,
            SMEM,
            SMEM,
            pl.BlockSpec((grids, tiles, pairs * cells, cells_x), lambda i: (0, i, 0, 0)),
            pl.BlockSpec((eofs.shape[0], tiles * cells_x), lambda i: (0, i)),
        ],
        out_specs=(
            pl.BlockSpec((grids, 3 * cap * cells, 2 * lanes), lambda i: (0, 0, 0)),
            pl.BlockSpec((cells, cap * eofs.shape[0]), lambda i: (0, 0)),
        ),
        scratch_shapes=[pltpu.SMEM((grids, 2 * cap), jnp.int32)]
        + [pltpu.VMEM(((3 * cap + 1) * cells, eofs.shape[0]), jnp.float32)] * grids,
        cost_estimate=pl.CostEstimate(
            flops=8 * flops, bytes_accessed=weights.size * 2, transcendentals=0
        ),
        compiler_params=grant(20),
        name="fold",
    )(requests, slots, counts, weights, eofs)


def times(source, folded):
    return lax.dot_general(
        source, folded, (((0,), (0,)), ((), ())), preferred_element_type=jnp.float32
    )


def near_kernel(requests, fields, others, a_ref, near_ref, kept_ref, order, chosen):
    _, lon, pair, cross, base, _ = place()
    grids, src_tiles, cells, columns = fields.shape
    cap = order.shape[0] - 1
    eofs = near_ref.shape[1]
    lanes = a_ref.shape[2] // 2
    for g in range(grids):
        for k, (owner, source) in enumerate(((lon, fields), (pair, others))):
            listed = list_tiles(requests, order, g, base + lon, base + owner, src_tiles)
            for j in range(cap):
                row = (k * cap + j) * cells
                chosen[row : row + cells, :] = source[g, listed[j]]
        total = times(chosen[...], a_ref[g, : 2 * cap * cells, :])
        near_ref[g * columns : (g + 1) * columns, :] = (
            total[:, :eofs] + total[:, lanes : lanes + eofs]
        )
    last = grids - 1
    for j, tile in enumerate(
        list_tiles(requests, order, last, base + cross, base + lon, src_tiles)
    ):
        kept_ref[j * cells : (j + 1) * cells, :] = fields[last, tile]


def near(requests, fields, others, folded, eofs):
    grids, _, cells, columns = fields.shape
    cap = requests.shape[1] // 2
    return pl.pallas_call(
        near_kernel,
        out_shape=(
            jax.ShapeDtypeStruct((grids * columns, eofs), jnp.float32),
            jax.ShapeDtypeStruct((cap * cells, columns), fields.dtype),
        ),
        in_specs=[SMEM, VMEM, VMEM, VMEM],
        out_specs=(VMEM, VMEM),
        scratch_shapes=[
            pltpu.SMEM((cap + 1,), jnp.int32),
            pltpu.VMEM((2 * cap * cells, columns), fields.dtype),
        ],
        cost_estimate=pl.CostEstimate(flops=10**9, bytes_accessed=10**6, transcendentals=0),
        compiler_params=grant(12),
        name="near",
    )(requests, fields, others, folded)


def far_kernel(
    lat_count, near_ref, tiles, kept, a_ref, others_ref, keep_ref, send_ref, rows_of, whole, units
):
    lat, lon, _, _, _, lon_count = place()
    grids, cap, cells, columns = tiles.shape[0] + 1, *tiles.shape[1:]
    eofs = near_ref.shape[1]
    lanes = a_ref.shape[2] // 2
    planes = lon_count // CORES
    rows = units.shape[1]
    for g in range(grids):
        part = slice(g * columns, (g + 1) * columns)
        if g < grids - 1:
            total = times(tiles[g].reshape(cap * cells, columns), a_ref[g, 2 * cap * cells :, :])
            total = total[:, :eofs] + total[:, lanes : lanes + eofs]
        else:
            for j in range(cap):
                rows_of[j * cells : (j + 1) * cells, :] = others_ref[:, j * eofs : (j + 1) * eofs]
            total = times(kept[...], rows_of[...])
        product = near_ref[part, :] + total
        product = product.reshape(columns // MONTHS, MONTHS, eofs)
        product = product - jnp.mean(product, axis=1, keepdims=True)
        whole[part, :] = product.reshape(columns, eofs)
    for u in range(units.shape[0]):
        units[u] = whole[u * rows : (u + 1) * rows, :]
    plane, core = lax.div(lon, CORES), lax.rem(lon, CORES)
    for c, out in ((0, keep_ref), (1, send_ref)):
        for r in range(planes):
            for q in range(lat_count):
                target = jnp.bitwise_xor(lat, q) * lon_count
                target += jnp.bitwise_xor(plane, r) * CORES + jnp.bitwise_xor(core, c)
                out[r, q * rows : (q + 1) * rows, :] = units[target]


def far(near_part, tiles, kept, folded, others):
    lat_count, lon_count = lax.axis_size("lat"), lax.axis_size("lon")
    total_columns, eofs = near_part.shape
    rows = total_columns // (lat_count * lon_count)
    block = jax.ShapeDtypeStruct((lon_count // CORES, lat_count * rows, eofs), jnp.float32)
    return pl.pallas_call(
        functools.partial(far_kernel, lat_count),
        out_shape=(block, block),
        in_specs=[VMEM] * 5,
        out_specs=(VMEM, VMEM),
        scratch_shapes=[
            pltpu.VMEM((kept.shape[0], eofs), others.dtype),
            pltpu.VMEM((total_columns, eofs), jnp.float32),
            pltpu.VMEM((lat_count * lon_count, rows, eofs), jnp.float32),
        ],
        compiler_params=grant(16),
        name="far",
    )(near_part, tiles, kept, folded, others)


def shards(fields, weights, pair_slots, pair_counts, requests, eofs):
    lat_count, lon_count = lax.axis_size("lat"), lax.axis_size("lon")
    planes = lon_count // CORES
    requests = stay(requests.transpose(0, 2, 1))
    pair_slots = stay(pair_slots.transpose(0, 2, 1))
    pair_counts = stay(pair_counts)
    eofs = stay(eofs)
    on_chip = [(i, i ^ 1) for i in range(lon_count)]
    off_chip = [(i, (i + 2 * (i % CORES) - 1) % lon_count) for i in range(lon_count)]
    picked, later = lax.optimization_barrier((pick(requests, stay(fields)), fields))
    tiles = lax.ppermute(picked, "lon", off_chip)
    others = lax.ppermute(later, "lon", on_chip)
    folded, spread = fold(requests, pair_slots, pair_counts, weights, eofs, fields.shape[1])
    spread = lax.ppermute(spread, "lon", off_chip)
    near_part, kept = near(requests, fields, others, folded, eofs.shape[0])
    keep, send = far(near_part, tiles, kept, folded, spread)
    pair_sum = keep + lax.ppermute(send, "lon", on_chip)
    plane_sum = pair_sum[0]
    for r in reversed(range(1, planes)):
        swap = [(i, i ^ (r * CORES)) for i in range(lon_count)]
        sent = lax.ppermute(pair_sum[r].astype(jnp.bfloat16), "lon", swap)
        plane_sum = plane_sum + sent.astype(jnp.float32)
    rows = plane_sum.shape[0] // lat_count
    total = plane_sum[:rows]
    for q in reversed(range(1, lat_count)):
        swap = [(i, i ^ q) for i in range(lat_count)]
        total = total + lax.ppermute(plane_sum[q * rows : (q + 1) * rows], "lat", swap)
    return total.T


def solution(mesh):
    return jax.shard_map(
        shards,
        mesh=mesh,
        in_specs=(
            P(None, ("lat", "lon"), None, None),
            P(None, ("lat", "lon"), None, None, None),
            P(None, ("lat", "lon"), None),
            P(None, ("lat", "lon")),
            P(),
            P(None, ("lat", "lon")),
        ),
        out_specs=P(None, ("lat", "lon")),
        check_vma=False,
    )
```

```python
import functools

import jax
import jax.numpy as jnp
from jax import lax
from jax.experimental import pallas as pl
from jax.experimental.pallas import tpu as pltpu
from jax.sharding import PartitionSpec as P


MONTHS = 24
CORES = 2
MIB = 2**20

SMEM = pl.BlockSpec(memory_space=pltpu.SMEM)
VMEM = pl.BlockSpec(memory_space=pltpu.VMEM)
HBM = pl.BlockSpec(memory_space=pl.ANY)


def grant(size):
    return pltpu.CompilerParams(vmem_limit_bytes=size * MIB)


def stay(array):
    return pltpu.with_memory_space_constraint(array, pltpu.HBM)


def place():
    lat, lon, lon_count = lax.axis_index("lat"), lax.axis_index("lon"), lax.axis_size("lon")
    core = lax.rem(lon, CORES)
    pair = lon + 1 - 2 * core
    cross = lax.rem(lon + 2 * core - 1 + lon_count, lon_count)
    return lat, lon, pair, cross, lat * lon_count, lon_count


def list_tiles(requests, order, g, reader, owner, src_tiles):
    rank = jnp.int32(0)
    for r in range(requests.shape[1]):
        local = requests[g, r, reader] - owner * src_tiles
        hit = jnp.logical_and(local >= 0, local < src_tiles)
        order[rank] = jnp.where(hit, local, 0)
        rank += hit.astype(jnp.int32)
    return [jnp.where(j < rank, order[j], 0) for j in range(order.shape[0] - 1)]


def pick_kernel(requests_ref, fields_ref, sent_ref, requests, fields, sems, *orders):
    _, lon, _, cross, base, _ = place()
    grids, src_tiles = fields.shape[:2]
    listing = pltpu.make_async_copy(requests_ref.at[:grids], requests, sems.at[grids])
    listing.start()
    loads = [pltpu.make_async_copy(fields_ref.at[g], fields.at[g], sems.at[g]) for g in range(grids)]
    for load in loads:
        load.start()
    listing.wait()
    listed = [
        list_tiles(requests, orders[g], g, base + cross, base + lon, src_tiles) for g in range(grids)
    ]
    for g in range(grids):
        loads[g].wait()
        for j, tile in enumerate(listed[g]):
            sent_ref[g, j] = fields[g, tile]


def pick(requests, fields):
    grids, src_tiles, cells, columns = fields.shape
    grids -= 1
    cap = requests.shape[1] // 2
    return pl.pallas_call(
        pick_kernel,
        out_shape=jax.ShapeDtypeStruct((grids, cap, cells, columns), fields.dtype),
        in_specs=[HBM, HBM],
        out_specs=VMEM,
        scratch_shapes=[
            pltpu.SMEM((grids, *requests.shape[1:]), jnp.int32),
            pltpu.VMEM((grids, src_tiles, cells, columns), fields.dtype),
            pltpu.SemaphoreType.DMA((grids + 1,)),
        ]
        + [pltpu.SMEM((cap + 1,), jnp.int32)] * grids,
        compiler_params=grant(6),
        name="pick",
    )(requests, fields)


def fold_kernel(
    src_tiles, first, sends, requests, slots_ref, counts_ref, w_ref, e_ref, a_ref, *rest
):
    sent_ref, where, *totals = rest if sends else (None, *rest)
    step = pl.program_id(0)
    grids, tiles, depth, cells_x = w_ref.shape
    slots = requests.shape[1]
    cap = slots // 2
    pairs = slots_ref.shape[1]
    cells = depth // pairs
    eofs = e_ref.shape[0]
    lanes = a_ref.shape[2] // 2
    chains = len(totals) // grids
    _, lon, pair, _, base, _ = place()

    @pl.when(step == 0)
    def _():
        for total in totals:
            total[...] = jnp.zeros_like(total)
        for g in range(grids):
            ranks = [jnp.int32(0)] * 3
            for r in range(slots):
                owner = lax.div(requests[first + g, r, base + lon], src_tiles) - base
                hits = [(owner == k).astype(jnp.int32) for k in (lon, pair)]
                hits.append(1 - hits[0] - hits[1])
                where[g, r] = sum(h * (k * cap + n) for k, (h, n) in enumerate(zip(hits, ranks)))
                ranks = [n + h for n, h in zip(ranks, hits)]

    for t in range(tiles):
        tile = step * tiles + t
        basis = e_ref[:, t * cells_x : (t + 1) * cells_x]
        parts = [
            lax.dot_general(
                w_ref[g, t], basis, (((1,), (1,)), ((), ())), preferred_element_type=jnp.float32
            )
            for g in range(grids)
        ]
        for p in range(pairs):
            for g in range(grids):
                spot = where[g, slots_ref[first + g, p, tile]]
                spot = jnp.where(p < counts_ref[first + g, tile], spot, 3 * cap)
                rows = pl.ds(pl.multiple_of(spot * cells, cells), cells)
                total = totals[g * chains + p % chains]
                total[rows, :] += parts[g][p * cells : (p + 1) * cells]

    @pl.when(step == pl.num_programs(0) - 1)
    def _():
        for g in range(grids):
            own = totals[g * chains : (g + 1) * chains]
            total = sum(part[: 3 * cap * cells, :] for part in own)
            high = total.astype(jnp.bfloat16)
            low = (total - high.astype(jnp.float32)).astype(jnp.bfloat16)
            a_ref[g, :, :eofs] = high
            a_ref[g, :, lanes : lanes + eofs] = low
            if sends:
                for j in range(cap):
                    row = (2 * cap + j) * cells
                    sent_ref[:, j * eofs : (j + 1) * eofs] = high[row : row + cells, :]


def fold(requests, slots, counts, weights, eofs, src_tiles, first, grids, sends):
    tile_total, depth, cells_x = weights.shape[1:]
    cap = requests.shape[1] // 2
    cells = depth // slots.shape[1]
    lanes = pl.cdiv(eofs.shape[0], 128) * 128
    tiles = tile_total // 2
    chains = 2 if sends else 1
    flops = 2 * grids * tile_total * depth * cells_x * eofs.shape[0]
    shapes = [jax.ShapeDtypeStruct((grids, 3 * cap * cells, 2 * lanes), jnp.bfloat16)]
    blocks = [pl.BlockSpec((grids, 3 * cap * cells, 2 * lanes), lambda i: (0, 0, 0))]
    if sends:
        shapes.append(jax.ShapeDtypeStruct((cells, cap * eofs.shape[0]), jnp.bfloat16))
        blocks.append(pl.BlockSpec((cells, cap * eofs.shape[0]), lambda i: (0, 0)))
    return pl.pallas_call(
        functools.partial(fold_kernel, src_tiles, first, sends),
        out_shape=shapes,
        grid=(tile_total // tiles,),
        in_specs=[
            SMEM,
            SMEM,
            SMEM,
            pl.BlockSpec((grids, tiles, depth, cells_x), lambda i: (first // grids, i, 0, 0)),
            pl.BlockSpec((eofs.shape[0], tiles * cells_x), lambda i: (0, i)),
        ],
        out_specs=blocks,
        scratch_shapes=[pltpu.SMEM((grids, 2 * cap), jnp.int32)]
        + [pltpu.VMEM(((3 * cap + 1) * cells, eofs.shape[0]), jnp.float32)] * (grids * chains),
        cost_estimate=pl.CostEstimate(
            flops=8 * flops, bytes_accessed=grids * tile_total * depth * cells_x * 2, transcendentals=0
        ),
        compiler_params=grant(24),
        name="fold",
    )(requests, slots, counts, weights, eofs)


def times(source, folded):
    return lax.dot_general(
        source, folded, (((0,), (0,)), ((), ())), preferred_element_type=jnp.float32
    )


def near_kernel(requests, fields, others, a_ref, last_ref, near_ref, kept_ref, order, chosen):
    _, lon, pair, cross, base, _ = place()
    grids, src_tiles, cells, columns = fields.shape
    cap = order.shape[0] - 1
    eofs = near_ref.shape[1]
    lanes = a_ref.shape[2] // 2
    for g in range(grids):
        for k, (owner, source) in enumerate(((lon, fields), (pair, others))):
            listed = list_tiles(requests, order, g, base + lon, base + owner, src_tiles)
            for j in range(cap):
                row = (k * cap + j) * cells
                chosen[row : row + cells, :] = source[g, listed[j]]
        weights = a_ref.at[g] if g < grids - 1 else last_ref.at[0]
        total = times(chosen[...], weights[: 2 * cap * cells, :])
        near_ref[g * columns : (g + 1) * columns, :] = (
            total[:, :eofs] + total[:, lanes : lanes + eofs]
        )
    last = grids - 1
    for j, tile in enumerate(
        list_tiles(requests, order, last, base + cross, base + lon, src_tiles)
    ):
        kept_ref[j * cells : (j + 1) * cells, :] = fields[last, tile]


def near(requests, fields, others, folded, last, eofs):
    grids, _, cells, columns = fields.shape
    cap = requests.shape[1] // 2
    return pl.pallas_call(
        near_kernel,
        out_shape=(
            jax.ShapeDtypeStruct((grids * columns, eofs), jnp.float32),
            jax.ShapeDtypeStruct((cap * cells, columns), fields.dtype),
        ),
        in_specs=[SMEM, VMEM, VMEM, VMEM, VMEM],
        out_specs=(VMEM, VMEM),
        scratch_shapes=[
            pltpu.SMEM((cap + 1,), jnp.int32),
            pltpu.VMEM((2 * cap * cells, columns), fields.dtype),
        ],
        cost_estimate=pl.CostEstimate(flops=10**9, bytes_accessed=10**6, transcendentals=0),
        compiler_params=grant(12),
        name="near",
    )(requests, fields, others, folded, last)


def far_kernel(
    lat_count, near_ref, tiles, kept, a_ref, others_ref, keep_ref, send_ref, rows_of, whole, units
):
    lat, lon, _, _, _, lon_count = place()
    grids, cap, cells, columns = tiles.shape[0] + 1, *tiles.shape[1:]
    eofs = near_ref.shape[1]
    lanes = a_ref.shape[2] // 2
    planes = lon_count // CORES
    rows = units.shape[1]
    for g in range(grids):
        part = slice(g * columns, (g + 1) * columns)
        if g < grids - 1:
            total = times(tiles[g].reshape(cap * cells, columns), a_ref[g, 2 * cap * cells :, :])
            total = total[:, :eofs] + total[:, lanes : lanes + eofs]
        else:
            for j in range(cap):
                rows_of[j * cells : (j + 1) * cells, :] = others_ref[:, j * eofs : (j + 1) * eofs]
            total = times(kept[...], rows_of[...])
        product = near_ref[part, :] + total
        product = product.reshape(columns // MONTHS, MONTHS, eofs)
        product = product - jnp.mean(product, axis=1, keepdims=True)
        whole[part, :] = product.reshape(columns, eofs)
    for u in range(units.shape[0]):
        units[u] = whole[u * rows : (u + 1) * rows, :]
    plane, core = lax.div(lon, CORES), lax.rem(lon, CORES)
    for c, out in ((0, keep_ref), (1, send_ref)):
        for r in range(planes):
            for q in range(lat_count):
                target = jnp.bitwise_xor(lat, q) * lon_count
                target += jnp.bitwise_xor(plane, r) * CORES + jnp.bitwise_xor(core, c)
                out[r, q * rows : (q + 1) * rows, :] = units[target]


def far(near_part, tiles, kept, folded, others):
    lat_count, lon_count = lax.axis_size("lat"), lax.axis_size("lon")
    total_columns, eofs = near_part.shape
    rows = total_columns // (lat_count * lon_count)
    block = jax.ShapeDtypeStruct((lon_count // CORES, lat_count * rows, eofs), jnp.float32)
    return pl.pallas_call(
        functools.partial(far_kernel, lat_count),
        out_shape=(block, block),
        in_specs=[VMEM] * 5,
        out_specs=(VMEM, VMEM),
        scratch_shapes=[
            pltpu.VMEM((kept.shape[0], eofs), others.dtype),
            pltpu.VMEM((total_columns, eofs), jnp.float32),
            pltpu.VMEM((lat_count * lon_count, rows, eofs), jnp.float32),
        ],
        compiler_params=grant(16),
        name="far",
    )(near_part, tiles, kept, folded, others)


def shards(fields, weights, pair_slots, pair_counts, requests, eofs):
    lat_count, lon_count = lax.axis_size("lat"), lax.axis_size("lon")
    planes = lon_count // CORES
    requests = stay(requests.transpose(0, 2, 1))
    pair_slots = stay(pair_slots.transpose(0, 2, 1))
    pair_counts = stay(pair_counts)
    eofs = stay(eofs)
    on_chip = [(i, i ^ 1) for i in range(lon_count)]
    off_chip = [(i, (i + 2 * (i % CORES) - 1) % lon_count) for i in range(lon_count)]
    picked, later = lax.optimization_barrier((pick(requests, stay(fields)), fields))
    tiles = lax.ppermute(picked, "lon", off_chip)
    others = lax.ppermute(later, "lon", on_chip)
    grids, tile_total, pairs, cells, cells_x = weights.shape
    weights = stay(weights.reshape(grids, tile_total, pairs * cells, cells_x))
    tables = (requests, pair_slots, pair_counts, weights, eofs, fields.shape[1])
    last, spread = fold(*tables, grids - 1, 1, True)
    spread = lax.ppermute(spread, "lon", off_chip)
    (folded,) = fold(*tables, 0, grids - 1, False)
    near_part, kept = near(requests, fields, others, folded, last, eofs.shape[0])
    keep, send = far(near_part, tiles, kept, folded, spread)
    pair_sum = keep + lax.ppermute(send, "lon", on_chip)
    plane_sum = pair_sum[0]
    for r in reversed(range(1, planes)):
        swap = [(i, i ^ (r * CORES)) for i in range(lon_count)]
        sent = lax.ppermute(pair_sum[r].astype(jnp.bfloat16), "lon", swap)
        plane_sum = plane_sum + sent.astype(jnp.float32)
    rows = plane_sum.shape[0] // lat_count
    total = plane_sum[:rows]
    for q in reversed(range(1, lat_count)):
        swap = [(i, i ^ q) for i in range(lat_count)]
        total = total + lax.ppermute(plane_sum[q * rows : (q + 1) * rows], "lat", swap)
    return total.T


def solution(mesh):
    return jax.shard_map(
        shards,
        mesh=mesh,
        in_specs=(
            P(None, ("lat", "lon"), None, None),
            P(None, ("lat", "lon"), None, None, None),
            P(None, ("lat", "lon"), None),
            P(None, ("lat", "lon")),
            P(),
            P(None, ("lat", "lon")),
        ),
        out_specs=P(None, ("lat", "lon")),
        check_vma=False,
    )
```

```python
import functools

import jax
import jax.numpy as jnp
from jax import lax
from jax.experimental import pallas as pl
from jax.experimental.pallas import tpu as pltpu
from jax.sharding import PartitionSpec as P


MONTHS = 24
CORES = 2
MIB = 2**20

SMEM = pl.BlockSpec(memory_space=pltpu.SMEM)
VMEM = pl.BlockSpec(memory_space=pltpu.VMEM)
HBM = pl.BlockSpec(memory_space=pl.ANY)


def grant(size):
    return pltpu.CompilerParams(vmem_limit_bytes=size * MIB)


def stay(array):
    return pltpu.with_memory_space_constraint(array, pltpu.HBM)


def place():
    lat, lon, lon_count = lax.axis_index("lat"), lax.axis_index("lon"), lax.axis_size("lon")
    core = lax.rem(lon, CORES)
    pair = lon + 1 - 2 * core
    cross = lax.rem(lon + 2 * core - 1 + lon_count, lon_count)
    return lat, lon, pair, cross, lat * lon_count, lon_count


def list_tiles(requests, order, g, reader, owner, src_tiles):
    rank = jnp.int32(0)
    for r in range(requests.shape[1]):
        local = requests[g, r, reader] - owner * src_tiles
        hit = jnp.logical_and(local >= 0, local < src_tiles)
        order[rank] = jnp.where(hit, local, 0)
        rank += hit.astype(jnp.int32)
    return [jnp.where(j < rank, order[j], 0) for j in range(order.shape[0] - 1)]


def pick_kernel(requests_ref, fields_ref, sent_ref, requests, fields, sems, *orders):
    _, lon, _, cross, base, _ = place()
    grids, src_tiles = fields.shape[:2]
    listing = pltpu.make_async_copy(requests_ref.at[:grids], requests, sems.at[grids])
    listing.start()
    loads = [pltpu.make_async_copy(fields_ref.at[g], fields.at[g], sems.at[g]) for g in range(grids)]
    for load in loads:
        load.start()
    listing.wait()
    listed = [
        list_tiles(requests, orders[g], g, base + cross, base + lon, src_tiles) for g in range(grids)
    ]
    for g in range(grids):
        loads[g].wait()
        for j, tile in enumerate(listed[g]):
            sent_ref[g, j] = fields[g, tile]


def pick(requests, fields):
    grids, src_tiles, cells, columns = fields.shape
    grids -= 1
    cap = requests.shape[1] // 2
    return pl.pallas_call(
        pick_kernel,
        out_shape=jax.ShapeDtypeStruct((grids, cap, cells, columns), fields.dtype),
        in_specs=[HBM, HBM],
        out_specs=VMEM,
        scratch_shapes=[
            pltpu.SMEM((grids, *requests.shape[1:]), jnp.int32),
            pltpu.VMEM((grids, src_tiles, cells, columns), fields.dtype),
            pltpu.SemaphoreType.DMA((grids + 1,)),
        ]
        + [pltpu.SMEM((cap + 1,), jnp.int32)] * grids,
        compiler_params=grant(6),
        name="pick",
    )(requests, fields)


def times(source, folded):
    return lax.dot_general(
        source, folded, (((0,), (0,)), ((), ())), preferred_element_type=jnp.float32
    )


def near_kernel(requests, fields, others, a_ref, last_ref, near_ref, kept_ref, order, chosen):
    _, lon, pair, cross, base, _ = place()
    grids, src_tiles, cells, columns = fields.shape
    cap = order.shape[0] - 1
    eofs = near_ref.shape[1]
    lanes = a_ref.shape[2] // 2
    for g in range(grids):
        for k, (owner, source) in enumerate(((lon, fields), (pair, others))):
            listed = list_tiles(requests, order, g, base + lon, base + owner, src_tiles)
            for j in range(cap):
                row = (k * cap + j) * cells
                chosen[row : row + cells, :] = source[g, listed[j]]
        weights = a_ref.at[g] if g < grids - 1 else last_ref.at[0]
        total = times(chosen[...], weights[: 2 * cap * cells, :])
        near_ref[g * columns : (g + 1) * columns, :] = (
            total[:, :eofs] + total[:, lanes : lanes + eofs]
        )
    last = grids - 1
    for j, tile in enumerate(
        list_tiles(requests, order, last, base + cross, base + lon, src_tiles)
    ):
        kept_ref[j * cells : (j + 1) * cells, :] = fields[last, tile]


def fold_kernel(
    src_tiles, first, sends, requests, slots_ref, counts_ref, w_ref, e_ref, *rest
):
    if sends:
        a_ref, sent_ref, where, *totals = rest
    else:
        fields, others, last_ref, a_ref, near_ref, kept_ref, where, order, chosen, *totals = rest
    step = pl.program_id(0)
    grids, tiles, depth, cells_x = w_ref.shape
    slots = requests.shape[1]
    cap = slots // 2
    pairs = slots_ref.shape[1]
    cells = depth // pairs
    eofs = e_ref.shape[0]
    lanes = a_ref.shape[2] // 2
    chains = len(totals) // grids
    _, lon, pair, _, base, _ = place()

    @pl.when(step == 0)
    def _():
        for total in totals:
            total[...] = jnp.zeros_like(total)
        for g in range(grids):
            ranks = [jnp.int32(0)] * 3
            for r in range(slots):
                owner = lax.div(requests[first + g, r, base + lon], src_tiles) - base
                hits = [(owner == k).astype(jnp.int32) for k in (lon, pair)]
                hits.append(1 - hits[0] - hits[1])
                where[g, r] = sum(h * (k * cap + n) for k, (h, n) in enumerate(zip(hits, ranks)))
                ranks = [n + h for n, h in zip(ranks, hits)]

    for t in range(tiles):
        tile = step * tiles + t
        basis = e_ref[:, t * cells_x : (t + 1) * cells_x]
        parts = [
            lax.dot_general(
                w_ref[g, t], basis, (((1,), (1,)), ((), ())), preferred_element_type=jnp.float32
            )
            for g in range(grids)
        ]
        for p in range(pairs):
            for g in range(grids):
                spot = where[g, slots_ref[first + g, p, tile]]
                spot = jnp.where(p < counts_ref[first + g, tile], spot, 3 * cap)
                rows = pl.ds(pl.multiple_of(spot * cells, cells), cells)
                total = totals[g * chains + p % chains]
                total[rows, :] += parts[g][p * cells : (p + 1) * cells]

    @pl.when(step == pl.num_programs(0) - 1)
    def _():
        for g in range(grids):
            own = totals[g * chains : (g + 1) * chains]
            total = sum(part[: 3 * cap * cells, :] for part in own)
            high = total.astype(jnp.bfloat16)
            low = (total - high.astype(jnp.float32)).astype(jnp.bfloat16)
            a_ref[g, :, :eofs] = high
            a_ref[g, :, lanes : lanes + eofs] = low
            if sends:
                for j in range(cap):
                    row = (2 * cap + j) * cells
                    sent_ref[:, j * eofs : (j + 1) * eofs] = high[row : row + cells, :]
        if not sends:
            near_kernel(
                requests, fields, others, a_ref, last_ref, near_ref, kept_ref, order, chosen
            )


def fold(requests, slots, counts, weights, eofs, src_tiles, first, grids, chip=None):
    sends = chip is None
    tile_total, depth, cells_x = weights.shape[1:]
    cap = requests.shape[1] // 2
    cells = depth // slots.shape[1]
    lanes = pl.cdiv(eofs.shape[0], 128) * 128
    tiles = tile_total // 2
    chains = 2 if sends else 1
    flops = 2 * grids * tile_total * depth * cells_x * eofs.shape[0]
    shapes = [jax.ShapeDtypeStruct((grids, 3 * cap * cells, 2 * lanes), jnp.bfloat16)]
    blocks = [pl.BlockSpec((grids, 3 * cap * cells, 2 * lanes), lambda i: (0, 0, 0))]
    if sends:
        shapes.append(jax.ShapeDtypeStruct((cells, cap * eofs.shape[0]), jnp.bfloat16))
        blocks.append(pl.BlockSpec((cells, cap * eofs.shape[0]), lambda i: (0, 0)))
    held = [pltpu.SMEM((grids, 2 * cap), jnp.int32)]
    if not sends:
        fields = chip[0]
        columns = fields.shape[3]
        shapes.append(jax.ShapeDtypeStruct((fields.shape[0] * columns, eofs.shape[0]), jnp.float32))
        shapes.append(jax.ShapeDtypeStruct((cap * cells, columns), fields.dtype))
        blocks += [VMEM, VMEM]
        held.append(pltpu.SMEM((cap + 1,), jnp.int32))
        held.append(pltpu.VMEM((2 * cap * cells, columns), fields.dtype))
    return pl.pallas_call(
        functools.partial(fold_kernel, src_tiles, first, sends),
        out_shape=shapes,
        grid=(tile_total // tiles,),
        in_specs=[
            SMEM,
            SMEM,
            SMEM,
            pl.BlockSpec((grids, tiles, depth, cells_x), lambda i: (first // grids, i, 0, 0)),
            pl.BlockSpec((eofs.shape[0], tiles * cells_x), lambda i: (0, i)),
        ]
        + [VMEM] * len(chip or ()),
        out_specs=blocks,
        scratch_shapes=held
        + [pltpu.VMEM(((3 * cap + 1) * cells, eofs.shape[0]), jnp.float32)] * (grids * chains),
        cost_estimate=pl.CostEstimate(
            flops=8 * flops, bytes_accessed=grids * tile_total * depth * cells_x * 2, transcendentals=0
        ),
        compiler_params=grant(24 if sends else 32),
        name="fold",
    )(requests, slots, counts, weights, eofs, *(chip or ()))


def far_kernel(
    lat_count, near_ref, tiles, kept, a_ref, others_ref, keep_ref, send_ref, rows_of, whole, units
):
    lat, lon, _, _, _, lon_count = place()
    grids, cap, cells, columns = tiles.shape[0] + 1, *tiles.shape[1:]
    eofs = near_ref.shape[1]
    lanes = a_ref.shape[2] // 2
    planes = lon_count // CORES
    rows = units.shape[1]
    for g in range(grids):
        part = slice(g * columns, (g + 1) * columns)
        if g < grids - 1:
            total = times(tiles[g].reshape(cap * cells, columns), a_ref[g, 2 * cap * cells :, :])
            total = total[:, :eofs] + total[:, lanes : lanes + eofs]
        else:
            for j in range(cap):
                rows_of[j * cells : (j + 1) * cells, :] = others_ref[:, j * eofs : (j + 1) * eofs]
            total = times(kept[...], rows_of[...])
        product = near_ref[part, :] + total
        product = product.reshape(columns // MONTHS, MONTHS, eofs)
        product = product - jnp.mean(product, axis=1, keepdims=True)
        whole[part, :] = product.reshape(columns, eofs)
    for u in range(units.shape[0]):
        units[u] = whole[u * rows : (u + 1) * rows, :]
    plane, core = lax.div(lon, CORES), lax.rem(lon, CORES)
    for c, out in ((0, keep_ref), (1, send_ref)):
        for r in range(planes):
            for q in range(lat_count):
                target = jnp.bitwise_xor(lat, q) * lon_count
                target += jnp.bitwise_xor(plane, r) * CORES + jnp.bitwise_xor(core, c)
                out[r, q * rows : (q + 1) * rows, :] = units[target]


def far(near_part, tiles, kept, folded, others):
    lat_count, lon_count = lax.axis_size("lat"), lax.axis_size("lon")
    total_columns, eofs = near_part.shape
    rows = total_columns // (lat_count * lon_count)
    block = jax.ShapeDtypeStruct((lon_count // CORES, lat_count * rows, eofs), jnp.float32)
    return pl.pallas_call(
        functools.partial(far_kernel, lat_count),
        out_shape=(block, block),
        in_specs=[VMEM] * 5,
        out_specs=(VMEM, VMEM),
        scratch_shapes=[
            pltpu.VMEM((kept.shape[0], eofs), others.dtype),
            pltpu.VMEM((total_columns, eofs), jnp.float32),
            pltpu.VMEM((lat_count * lon_count, rows, eofs), jnp.float32),
        ],
        compiler_params=grant(16),
        name="far",
    )(near_part, tiles, kept, folded, others)


def shards(fields, weights, pair_slots, pair_counts, requests, eofs):
    lat_count, lon_count = lax.axis_size("lat"), lax.axis_size("lon")
    planes = lon_count // CORES
    requests = stay(requests.transpose(0, 2, 1))
    pair_slots = stay(pair_slots.transpose(0, 2, 1))
    pair_counts = stay(pair_counts)
    eofs = stay(eofs)
    on_chip = [(i, i ^ 1) for i in range(lon_count)]
    off_chip = [(i, (i + 2 * (i % CORES) - 1) % lon_count) for i in range(lon_count)]
    picked, later = lax.optimization_barrier((pick(requests, stay(fields)), fields))
    tiles = lax.ppermute(picked, "lon", off_chip)
    others = lax.ppermute(later, "lon", on_chip)
    grids, tile_total, pairs, cells, cells_x = weights.shape
    weights = stay(weights.reshape(grids, tile_total, pairs * cells, cells_x))
    tables = (requests, pair_slots, pair_counts, weights, eofs, fields.shape[1])
    last, spread = fold(*tables, grids - 1, 1)
    spread = lax.ppermute(spread, "lon", off_chip)
    folded, near_part, kept = fold(*tables, 0, grids - 1, (fields, others, last))
    keep, send = far(near_part, tiles, kept, folded, spread)
    pair_sum = keep + lax.ppermute(send, "lon", on_chip)
    plane_sum = pair_sum[0]
    for r in reversed(range(1, planes)):
        swap = [(i, i ^ (r * CORES)) for i in range(lon_count)]
        sent = lax.ppermute(pair_sum[r].astype(jnp.bfloat16), "lon", swap)
        plane_sum = plane_sum + sent.astype(jnp.float32)
    rows = plane_sum.shape[0] // lat_count
    total = plane_sum[:rows]
    for q in reversed(range(1, lat_count)):
        swap = [(i, i ^ q) for i in range(lat_count)]
        total = total + lax.ppermute(plane_sum[q * rows : (q + 1) * rows], "lat", swap)
    return total.T


def solution(mesh):
    return jax.shard_map(
        shards,
        mesh=mesh,
        in_specs=(
            P(None, ("lat", "lon"), None, None),
            P(None, ("lat", "lon"), None, None, None),
            P(None, ("lat", "lon"), None),
            P(None, ("lat", "lon")),
            P(),
            P(None, ("lat", "lon")),
        ),
        out_specs=P(None, ("lat", "lon")),
        check_vma=False,
    )
```

```python
import functools

import jax
import jax.numpy as jnp
from jax import lax
from jax.experimental import pallas as pl
from jax.experimental.pallas import tpu as pltpu
from jax.sharding import PartitionSpec as P


MONTHS = 24
CORES = 2
SIDE = 3
MIB = 2**20

SMEM = pl.BlockSpec(memory_space=pltpu.SMEM)
VMEM = pl.BlockSpec(memory_space=pltpu.VMEM)
HBM = pl.BlockSpec(memory_space=pl.ANY)


def grant(size):
    return pltpu.CompilerParams(vmem_limit_bytes=size * MIB)


def stay(array):
    return pltpu.with_memory_space_constraint(array, pltpu.HBM)


def place():
    lat, lon, lon_count = lax.axis_index("lat"), lax.axis_index("lon"), lax.axis_size("lon")
    core = lax.rem(lon, CORES)
    pair = lon + 1 - 2 * core
    cross = lax.rem(lon + 2 * core - 1 + lon_count, lon_count)
    return lat, lon, pair, cross, lat * lon_count, lon_count


def list_tiles(requests, order, g, reader, owner, src_tiles):
    rank = jnp.int32(0)
    for r in range(requests.shape[1]):
        local = requests[g, r, reader] - owner * src_tiles
        hit = jnp.logical_and(local >= 0, local < src_tiles)
        order[rank] = jnp.where(hit, local, 0)
        rank += hit.astype(jnp.int32)
    return [jnp.where(j < rank, order[j], 0) for j in range(order.shape[0] - 1)]


def pick_kernel(requests_ref, fields_ref, sent_ref, requests, fields, sems, *orders):
    _, lon, _, cross, base, _ = place()
    grids, src_tiles = fields.shape[:2]
    listing = pltpu.make_async_copy(requests_ref.at[:grids], requests, sems.at[grids])
    listing.start()
    loads = [pltpu.make_async_copy(fields_ref.at[g], fields.at[g], sems.at[g]) for g in range(grids)]
    for load in loads:
        load.start()
    listing.wait()
    listed = [
        list_tiles(requests, orders[g], g, base + cross, base + lon, src_tiles) for g in range(grids)
    ]
    for g in range(grids):
        loads[g].wait()
        for j, tile in enumerate(listed[g]):
            sent_ref[g, j] = fields[g, tile]


def pick(requests, fields):
    grids, src_tiles, cells, columns = fields.shape
    grids -= 1
    cap = requests.shape[1] // 2
    return pl.pallas_call(
        pick_kernel,
        out_shape=jax.ShapeDtypeStruct((grids, cap, cells, columns), fields.dtype),
        in_specs=[HBM, HBM],
        out_specs=VMEM,
        scratch_shapes=[
            pltpu.SMEM((grids, *requests.shape[1:]), jnp.int32),
            pltpu.VMEM((grids, src_tiles, cells, columns), fields.dtype),
            pltpu.SemaphoreType.DMA((grids + 1,)),
        ]
        + [pltpu.SMEM((cap + 1,), jnp.int32)] * grids,
        compiler_params=grant(6),
        name="pick",
    )(requests, fields)


def times(source, folded):
    return lax.dot_general(
        source, folded, (((0,), (0,)), ((), ())), preferred_element_type=jnp.float32
    )


def near_kernel(requests, fields, others, a_ref, last_ref, near_ref, kept_ref, order, chosen):
    _, lon, pair, cross, base, _ = place()
    grids, src_tiles, cells, columns = fields.shape
    cap = order.shape[0] - 1
    eofs = near_ref.shape[1]
    lanes = a_ref.shape[2] // 2
    for g in range(grids):
        for k, (owner, source) in enumerate(((lon, fields), (pair, others))):
            listed = list_tiles(requests, order, g, base + lon, base + owner, src_tiles)
            for j in range(cap):
                row = (k * cap + j) * cells
                chosen[row : row + cells, :] = source[g, listed[j]]
        weights = a_ref.at[g] if g < grids - 1 else last_ref.at[0]
        total = times(chosen[...], weights[: 2 * cap * cells, :])
        near_ref[g * columns : (g + 1) * columns, :] = (
            total[:, :eofs] + total[:, lanes : lanes + eofs]
        )
    last = grids - 1
    for j, tile in enumerate(
        list_tiles(requests, order, last, base + cross, base + lon, src_tiles)
    ):
        kept_ref[j * cells : (j + 1) * cells, :] = fields[last, tile]


def fold_kernel(
    src_tiles, first, sends, requests, slots_ref, counts_ref, w_ref, e_ref, *rest
):
    if sends:
        a_ref, sent_ref, where, *totals = rest
    else:
        fields, others, last_ref, a_ref, near_ref, kept_ref, where, order, chosen, *totals = rest
    step = pl.program_id(0)
    grids, tiles, depth, cells_x = w_ref.shape
    slots = requests.shape[1]
    cap = slots // 2
    pairs = slots_ref.shape[1]
    cells = depth // pairs
    eofs = e_ref.shape[0]
    lanes = a_ref.shape[2] // 2
    chains = len(totals) // grids
    _, lon, pair, _, base, _ = place()

    @pl.when(step == 0)
    def _():
        for total in totals:
            total[...] = jnp.zeros_like(total)
        for g in range(grids):
            ranks = [jnp.int32(0)] * 3
            for r in range(slots):
                owner = lax.div(requests[first + g, r, base + lon], src_tiles) - base
                hits = [(owner == k).astype(jnp.int32) for k in (lon, pair)]
                hits.append(1 - hits[0] - hits[1])
                where[g, r] = sum(h * (k * cap + n) for k, (h, n) in enumerate(zip(hits, ranks)))
                ranks = [n + h for n, h in zip(ranks, hits)]

    for t in range(tiles):
        tile = step * tiles + t
        basis = e_ref[:, t * cells_x : (t + 1) * cells_x]
        parts = [
            lax.dot_general(
                w_ref[g, t], basis, (((1,), (1,)), ((), ())), preferred_element_type=jnp.float32
            )
            for g in range(grids)
        ]
        for p in range(pairs):
            for g in range(grids):
                spot = where[g, slots_ref[first + g, p, tile]]
                spot = jnp.where(p < counts_ref[first + g, tile], spot, 3 * cap)
                rows = pl.ds(pl.multiple_of(spot * cells, cells), cells)
                total = totals[g * chains + p % chains]
                total[rows, :] += parts[g][p * cells : (p + 1) * cells]

    @pl.when(step == pl.num_programs(0) - 1)
    def _():
        for g in range(grids):
            own = totals[g * chains : (g + 1) * chains]
            total = sum(part[: 3 * cap * cells, :] for part in own)
            high = total.astype(jnp.bfloat16)
            low = (total - high.astype(jnp.float32)).astype(jnp.bfloat16)
            a_ref[g, :, :eofs] = high
            a_ref[g, :, lanes : lanes + eofs] = low
            if sends:
                for j in range(cap):
                    row = (2 * cap + j) * cells
                    sent_ref[:, j * eofs : (j + 1) * eofs] = high[row : row + cells, :]
        if not sends:
            near_kernel(
                requests, fields, others, a_ref, last_ref, near_ref, kept_ref, order, chosen
            )


def fold(requests, slots, counts, weights, eofs, src_tiles, first, grids, chip=None):
    sends = chip is None
    tile_total, depth, cells_x = weights.shape[1:]
    cap = requests.shape[1] // 2
    cells = depth // slots.shape[1]
    lanes = pl.cdiv(eofs.shape[0], 128) * 128
    tiles = tile_total // 2
    chains = 2 if sends else 1
    flops = 2 * grids * tile_total * depth * cells_x * eofs.shape[0]
    shapes = [jax.ShapeDtypeStruct((grids, 3 * cap * cells, 2 * lanes), jnp.bfloat16)]
    blocks = [pl.BlockSpec((grids, 3 * cap * cells, 2 * lanes), lambda i: (0, 0, 0))]
    if sends:
        shapes.append(jax.ShapeDtypeStruct((cells, cap * eofs.shape[0]), jnp.bfloat16))
        blocks.append(pl.BlockSpec((cells, cap * eofs.shape[0]), lambda i: (0, 0)))
    held = [pltpu.SMEM((grids, 2 * cap), jnp.int32)]
    if not sends:
        fields = chip[0]
        columns = fields.shape[3]
        shapes.append(jax.ShapeDtypeStruct((fields.shape[0] * columns, eofs.shape[0]), jnp.float32))
        shapes.append(jax.ShapeDtypeStruct((cap * cells, columns), fields.dtype))
        blocks += [VMEM, VMEM]
        held.append(pltpu.SMEM((cap + 1,), jnp.int32))
        held.append(pltpu.VMEM((2 * cap * cells, columns), fields.dtype))
    return pl.pallas_call(
        functools.partial(fold_kernel, src_tiles, first, sends),
        out_shape=shapes,
        grid=(tile_total // tiles,),
        in_specs=[
            SMEM,
            SMEM,
            SMEM,
            pl.BlockSpec((grids, tiles, depth, cells_x), lambda i: (first // grids, i, 0, 0)),
            pl.BlockSpec((eofs.shape[0], tiles * cells_x), lambda i: (0, i)),
        ]
        + [VMEM] * len(chip or ()),
        out_specs=blocks,
        scratch_shapes=held
        + [pltpu.VMEM(((3 * cap + 1) * cells, eofs.shape[0]), jnp.float32)] * (grids * chains),
        cost_estimate=pl.CostEstimate(
            flops=8 * flops, bytes_accessed=grids * tile_total * depth * cells_x * 2, transcendentals=0
        ),
        compiler_params=grant(24 if sends else 32),
        name="fold",
    )(requests, slots, counts, weights, eofs, *(chip or ()))


def far_kernel(
    lat_count, near_ref, tiles, kept, a_ref, others_ref, keep_ref, send_ref, rows_of, whole, units
):
    lat, lon, _, _, _, lon_count = place()
    grids, cap, cells, columns = tiles.shape[0] + 1, *tiles.shape[1:]
    eofs = near_ref.shape[1]
    lanes = a_ref.shape[2] // 2
    planes = lon_count // CORES
    rows = units.shape[1]
    part_rows = keep_ref.shape[1] // lat_count
    side = rows // part_rows
    for g in range(grids):
        part = slice(g * columns, (g + 1) * columns)
        if g < grids - 1:
            total = times(tiles[g].reshape(cap * cells, columns), a_ref[g, 2 * cap * cells :, :])
            total = total[:, :eofs] + total[:, lanes : lanes + eofs]
        else:
            for j in range(cap):
                rows_of[j * cells : (j + 1) * cells, :] = others_ref[:, j * eofs : (j + 1) * eofs]
            total = times(kept[...], rows_of[...])
        product = near_ref[part, :] + total
        product = product.reshape(columns // MONTHS, MONTHS, eofs)
        product = product - jnp.mean(product, axis=1, keepdims=True)
        whole[part, :] = product.reshape(columns, eofs)
    for u in range(units.shape[0]):
        units[u] = whole[u * rows : (u + 1) * rows, :]
    plane, core = lax.div(lon, CORES), lax.rem(lon, CORES)
    for c, out in ((0, keep_ref), (1, send_ref)):
        for r in range(planes):
            for q in range(lat_count):
                target = jnp.bitwise_xor(lat, q) * lon_count
                target += jnp.bitwise_xor(plane, r) * CORES + jnp.bitwise_xor(core, c)
                for i in range(side):
                    piece = units[target, i * part_rows : (i + 1) * part_rows, :]
                    out[r, q * part_rows : (q + 1) * part_rows, i * eofs : (i + 1) * eofs] = piece


def far(near_part, tiles, kept, folded, others):
    lat_count, lon_count = lax.axis_size("lat"), lax.axis_size("lon")
    total_columns, eofs = near_part.shape
    rows = total_columns // (lat_count * lon_count)
    side = SIDE if rows % SIDE == 0 else 1
    shape = (lon_count // CORES, lat_count * rows // side, side * eofs)
    block = jax.ShapeDtypeStruct(shape, jnp.float32)
    return pl.pallas_call(
        functools.partial(far_kernel, lat_count),
        out_shape=(block, block),
        in_specs=[VMEM] * 5,
        out_specs=(VMEM, VMEM),
        scratch_shapes=[
            pltpu.VMEM((kept.shape[0], eofs), others.dtype),
            pltpu.VMEM((total_columns, eofs), jnp.float32),
            pltpu.VMEM((lat_count * lon_count, rows, eofs), jnp.float32),
        ],
        compiler_params=grant(16),
        name="far",
    )(near_part, tiles, kept, folded, others)


def finish_kernel(*refs):
    *parts, out_ref = refs
    total = sum(part[...] for part in parts)
    rows, eofs = parts[0].shape[0], out_ref.shape[1]
    for i in range(out_ref.shape[0] // rows):
        out_ref[i * rows : (i + 1) * rows, :] = total[:, i * eofs : (i + 1) * eofs]


def finish(parts, eofs):
    size = parts[0].size // eofs
    return pl.pallas_call(
        finish_kernel,
        out_shape=jax.ShapeDtypeStruct((size, eofs), jnp.float32),
        in_specs=[VMEM] * len(parts),
        out_specs=VMEM,
        compiler_params=grant(2),
        name="finish",
    )(*parts)


def shards(fields, weights, pair_slots, pair_counts, requests, eofs):
    lat_count, lon_count = lax.axis_size("lat"), lax.axis_size("lon")
    planes = lon_count // CORES
    requests = stay(requests.transpose(0, 2, 1))
    pair_slots = stay(pair_slots.transpose(0, 2, 1))
    pair_counts = stay(pair_counts)
    eofs = stay(eofs)
    on_chip = [(i, i ^ 1) for i in range(lon_count)]
    off_chip = [(i, (i + 2 * (i % CORES) - 1) % lon_count) for i in range(lon_count)]
    picked, later = lax.optimization_barrier((pick(requests, stay(fields)), fields))
    tiles = lax.ppermute(picked, "lon", off_chip)
    others = lax.ppermute(later, "lon", on_chip)
    grids, tile_total, pairs, cells, cells_x = weights.shape
    weights = stay(weights.reshape(grids, tile_total, pairs * cells, cells_x))
    tables = (requests, pair_slots, pair_counts, weights, eofs, fields.shape[1])
    last, spread = fold(*tables, grids - 1, 1)
    spread = lax.ppermute(spread, "lon", off_chip)
    folded, near_part, kept = fold(*tables, 0, grids - 1, (fields, others, last))
    keep, send = far(near_part, tiles, kept, folded, spread)
    pair_sum = keep + lax.ppermute(send, "lon", on_chip)
    plane_sum = pair_sum[0]
    for r in reversed(range(1, planes)):
        swap = [(i, i ^ (r * CORES)) for i in range(lon_count)]
        sent = lax.ppermute(pair_sum[r].astype(jnp.bfloat16), "lon", swap)
        plane_sum = plane_sum + sent.astype(jnp.float32)
    rows = plane_sum.shape[0] // lat_count
    parts = [plane_sum[:rows]]
    for q in reversed(range(1, lat_count)):
        swap = [(i, i ^ q) for i in range(lat_count)]
        parts.append(lax.ppermute(plane_sum[q * rows : (q + 1) * rows], "lat", swap))
    return finish(parts, eofs.shape[0]).T


def solution(mesh):
    return jax.shard_map(
        shards,
        mesh=mesh,
        in_specs=(
            P(None, ("lat", "lon"), None, None),
            P(None, ("lat", "lon"), None, None, None),
            P(None, ("lat", "lon"), None),
            P(None, ("lat", "lon")),
            P(),
            P(None, ("lat", "lon")),
        ),
        out_specs=P(None, ("lat", "lon")),
        check_vma=False,
    )
```

```python
import functools

import jax
import jax.numpy as jnp
from jax import lax
from jax.experimental import pallas as pl
from jax.experimental.pallas import tpu as pltpu
from jax.sharding import PartitionSpec as P


MONTHS = 24
CORES = 2
SIDE = 3
MIB = 2**20

SMEM = pl.BlockSpec(memory_space=pltpu.SMEM)
VMEM = pl.BlockSpec(memory_space=pltpu.VMEM)
HBM = pl.BlockSpec(memory_space=pl.ANY)


def grant(size):
    return pltpu.CompilerParams(vmem_limit_bytes=size * MIB)


def stay(array):
    return pltpu.with_memory_space_constraint(array, pltpu.HBM)


def place():
    lat, lon, lon_count = lax.axis_index("lat"), lax.axis_index("lon"), lax.axis_size("lon")
    core = lax.rem(lon, CORES)
    pair = lon + 1 - 2 * core
    cross = lax.rem(lon + 2 * core - 1 + lon_count, lon_count)
    return lat, lon, pair, cross, lat * lon_count, lon_count


def list_tiles(requests, order, g, reader, owner, src_tiles):
    rank = jnp.int32(0)
    for r in range(requests.shape[1]):
        local = requests[g, r, reader] - owner * src_tiles
        hit = jnp.logical_and(local >= 0, local < src_tiles)
        order[rank] = jnp.where(hit, local, 0)
        rank += hit.astype(jnp.int32)
    return [jnp.where(j < rank, order[j], 0) for j in range(order.shape[0] - 1)]


def pick_kernel(requests_ref, fields_ref, sent_ref, requests, fields, sems, *orders):
    _, lon, _, cross, base, _ = place()
    grids, src_tiles = fields.shape[:2]
    listing = pltpu.make_async_copy(requests_ref.at[:grids], requests, sems.at[grids])
    listing.start()
    loads = [pltpu.make_async_copy(fields_ref.at[g], fields.at[g], sems.at[g]) for g in range(grids)]
    for load in loads:
        load.start()
    listing.wait()
    listed = [
        list_tiles(requests, orders[g], g, base + cross, base + lon, src_tiles) for g in range(grids)
    ]
    for g in range(grids):
        loads[g].wait()
        for j, tile in enumerate(listed[g]):
            sent_ref[g, j] = fields[g, tile]


def pick(requests, fields):
    grids, src_tiles, cells, columns = fields.shape
    grids -= 1
    cap = requests.shape[1] // 2
    return pl.pallas_call(
        pick_kernel,
        out_shape=jax.ShapeDtypeStruct((grids, cap, cells, columns), fields.dtype),
        in_specs=[HBM, HBM],
        out_specs=VMEM,
        scratch_shapes=[
            pltpu.SMEM((grids, *requests.shape[1:]), jnp.int32),
            pltpu.VMEM((grids, src_tiles, cells, columns), fields.dtype),
            pltpu.SemaphoreType.DMA((grids + 1,)),
        ]
        + [pltpu.SMEM((cap + 1,), jnp.int32)] * grids,
        compiler_params=grant(6),
        name="pick",
    )(requests, fields)


def times(source, folded):
    return lax.dot_general(
        source, folded, (((0,), (0,)), ((), ())), preferred_element_type=jnp.float32
    )


def near_kernel(requests, fields, others, a_ref, last_ref, near_ref, kept_ref, order, chosen):
    _, lon, pair, cross, base, _ = place()
    grids, src_tiles, cells, columns = fields.shape
    cap = order.shape[0] - 1
    eofs = near_ref.shape[1]
    lanes = a_ref.shape[2] // 2
    for g in range(grids):
        for k, (owner, source) in enumerate(((lon, fields), (pair, others))):
            listed = list_tiles(requests, order, g, base + lon, base + owner, src_tiles)
            for j in range(cap):
                row = (k * cap + j) * cells
                chosen[row : row + cells, :] = source[g, listed[j]]
        weights = a_ref.at[g] if g < grids - 1 else last_ref.at[0]
        total = times(chosen[...], weights[: 2 * cap * cells, :])
        near_ref[g * columns : (g + 1) * columns, :] = (
            total[:, :eofs] + total[:, lanes : lanes + eofs]
        )
    last = grids - 1
    for j, tile in enumerate(
        list_tiles(requests, order, last, base + cross, base + lon, src_tiles)
    ):
        kept_ref[j * cells : (j + 1) * cells, :] = fields[last, tile]


def fold_kernel(
    src_tiles, first, sends, requests, slots_ref, counts_ref, w_ref, e_ref, *rest
):
    if sends:
        a_ref, sent_ref, where, *totals = rest
    else:
        fields, others, last_ref, a_ref, near_ref, kept_ref, where, order, chosen, *totals = rest
    step = pl.program_id(0)
    grids, tiles, depth, cells_x = w_ref.shape
    slots = requests.shape[1]
    cap = slots // 2
    pairs = slots_ref.shape[1]
    cells = depth // pairs
    eofs = e_ref.shape[0]
    lanes = a_ref.shape[2] // 2
    chains = len(totals) // grids
    _, lon, pair, _, base, _ = place()

    @pl.when(step == 0)
    def _():
        for total in totals:
            total[...] = jnp.zeros_like(total)
        for g in range(grids):
            ranks = [jnp.int32(0)] * 3
            for r in range(slots):
                owner = lax.div(requests[first + g, r, base + lon], src_tiles) - base
                hits = [(owner == k).astype(jnp.int32) for k in (lon, pair)]
                hits.append(1 - hits[0] - hits[1])
                where[g, r] = sum(h * (k * cap + n) for k, (h, n) in enumerate(zip(hits, ranks)))
                ranks = [n + h for n, h in zip(ranks, hits)]

    for t in range(tiles):
        tile = step * tiles + t
        basis = e_ref[:, t * cells_x : (t + 1) * cells_x]
        parts = [
            lax.dot_general(
                w_ref[g, t], basis, (((1,), (1,)), ((), ())), preferred_element_type=jnp.float32
            )
            for g in range(grids)
        ]
        for p in range(pairs):
            for g in range(grids):
                spot = where[g, slots_ref[first + g, p, tile]]
                spot = jnp.where(p < counts_ref[first + g, tile], spot, 3 * cap)
                rows = pl.ds(pl.multiple_of(spot * cells, cells), cells)
                total = totals[g * chains + p % chains]
                total[rows, :] += parts[g][p * cells : (p + 1) * cells]

    @pl.when(step == pl.num_programs(0) - 1)
    def _():
        for g in range(grids):
            own = totals[g * chains : (g + 1) * chains]
            total = sum(part[: 3 * cap * cells, :] for part in own)
            high = total.astype(jnp.bfloat16)
            low = (total - high.astype(jnp.float32)).astype(jnp.bfloat16)
            a_ref[g, :, :eofs] = high
            a_ref[g, :, lanes : lanes + eofs] = low
            if sends:
                for j in range(cap):
                    row = (2 * cap + j) * cells
                    sent_ref[:, j * eofs : (j + 1) * eofs] = high[row : row + cells, :]
        if not sends:
            near_kernel(
                requests, fields, others, a_ref, last_ref, near_ref, kept_ref, order, chosen
            )


def fold(requests, slots, counts, weights, eofs, src_tiles, first, grids, chip=None):
    sends = chip is None
    tile_total, depth, cells_x = weights.shape[1:]
    cap = requests.shape[1] // 2
    cells = depth // slots.shape[1]
    lanes = pl.cdiv(eofs.shape[0], 128) * 128
    tiles = tile_total // 2
    chains = 2 if sends else 1
    flops = 2 * grids * tile_total * depth * cells_x * eofs.shape[0]
    shapes = [jax.ShapeDtypeStruct((grids, 3 * cap * cells, 2 * lanes), jnp.bfloat16)]
    blocks = [pl.BlockSpec((grids, 3 * cap * cells, 2 * lanes), lambda i: (0, 0, 0))]
    if sends:
        shapes.append(jax.ShapeDtypeStruct((cells, cap * eofs.shape[0]), jnp.bfloat16))
        blocks.append(pl.BlockSpec((cells, cap * eofs.shape[0]), lambda i: (0, 0)))
    held = [pltpu.SMEM((grids, 2 * cap), jnp.int32)]
    if not sends:
        fields = chip[0]
        columns = fields.shape[3]
        shapes.append(jax.ShapeDtypeStruct((fields.shape[0] * columns, eofs.shape[0]), jnp.float32))
        shapes.append(jax.ShapeDtypeStruct((cap * cells, columns), fields.dtype))
        blocks += [VMEM, VMEM]
        held.append(pltpu.SMEM((cap + 1,), jnp.int32))
        held.append(pltpu.VMEM((2 * cap * cells, columns), fields.dtype))
    return pl.pallas_call(
        functools.partial(fold_kernel, src_tiles, first, sends),
        out_shape=shapes,
        grid=(tile_total // tiles,),
        in_specs=[
            SMEM,
            SMEM,
            SMEM,
            pl.BlockSpec((grids, tiles, depth, cells_x), lambda i: (first // grids, i, 0, 0)),
            pl.BlockSpec((eofs.shape[0], tiles * cells_x), lambda i: (0, i)),
        ]
        + [VMEM] * len(chip or ()),
        out_specs=blocks,
        scratch_shapes=held
        + [pltpu.VMEM(((3 * cap + 1) * cells, eofs.shape[0]), jnp.float32)] * (grids * chains),
        cost_estimate=pl.CostEstimate(
            flops=8 * flops, bytes_accessed=grids * tile_total * depth * cells_x * 2, transcendentals=0
        ),
        compiler_params=grant(24 if sends else 32),
        name="fold",
    )(requests, slots, counts, weights, eofs, *(chip or ()))


def far_kernel(
    lat_count, near_ref, tiles, kept, a_ref, others_ref, keep_ref, send_ref, rows_of, units
):
    lat, lon, _, _, _, lon_count = place()
    grids, cap, cells, columns = tiles.shape[0] + 1, *tiles.shape[1:]
    eofs = near_ref.shape[1]
    lanes = a_ref.shape[2] // 2
    planes = lon_count // CORES
    rows = units.shape[1]
    part_rows = keep_ref.shape[1] // lat_count
    side = rows // part_rows
    for g in range(grids):
        part = slice(g * columns, (g + 1) * columns)
        if g < grids - 1:
            total = times(tiles[g].reshape(cap * cells, columns), a_ref[g, 2 * cap * cells :, :])
            total = total[:, :eofs] + total[:, lanes : lanes + eofs]
        else:
            for j in range(cap):
                rows_of[j * cells : (j + 1) * cells, :] = others_ref[:, j * eofs : (j + 1) * eofs]
            total = times(kept[...], rows_of[...])
        product = near_ref[part, :] + total
        product = product.reshape(columns // MONTHS, MONTHS, eofs)
        product = product - jnp.mean(product, axis=1, keepdims=True)
        product = product.reshape(columns, eofs)
        for u in range(part.start // rows, pl.cdiv(part.stop, rows)):
            low, high = max(part.start, u * rows), min(part.stop, (u + 1) * rows)
            piece = product[low - part.start : high - part.start, :]
            units[u, low - u * rows : high - u * rows, :] = piece
    plane, core = lax.div(lon, CORES), lax.rem(lon, CORES)
    for c, out in ((0, keep_ref), (1, send_ref)):
        for r in range(planes):
            for q in range(lat_count):
                target = jnp.bitwise_xor(lat, q) * lon_count
                target += jnp.bitwise_xor(plane, r) * CORES + jnp.bitwise_xor(core, c)
                for i in range(side):
                    piece = units[target, i * part_rows : (i + 1) * part_rows, :]
                    out[r, q * part_rows : (q + 1) * part_rows, i * eofs : (i + 1) * eofs] = piece


def far(near_part, tiles, kept, folded, others):
    lat_count, lon_count = lax.axis_size("lat"), lax.axis_size("lon")
    total_columns, eofs = near_part.shape
    rows = total_columns // (lat_count * lon_count)
    side = SIDE if rows % SIDE == 0 else 1
    shape = (lon_count // CORES, lat_count * rows // side, side * eofs)
    block = jax.ShapeDtypeStruct(shape, jnp.float32)
    return pl.pallas_call(
        functools.partial(far_kernel, lat_count),
        out_shape=(block, block),
        in_specs=[VMEM] * 5,
        out_specs=(VMEM, VMEM),
        scratch_shapes=[
            pltpu.VMEM((kept.shape[0], eofs), others.dtype),
            pltpu.VMEM((lat_count * lon_count, rows, eofs), jnp.float32),
        ],
        compiler_params=grant(16),
        name="far",
    )(near_part, tiles, kept, folded, others)


def finish_kernel(*refs):
    *parts, out_ref = refs
    total = sum(part[...] for part in parts)
    rows, eofs = parts[0].shape[0], out_ref.shape[1]
    for i in range(out_ref.shape[0] // rows):
        out_ref[i * rows : (i + 1) * rows, :] = total[:, i * eofs : (i + 1) * eofs]


def finish(parts, eofs):
    size = parts[0].size // eofs
    return pl.pallas_call(
        finish_kernel,
        out_shape=jax.ShapeDtypeStruct((size, eofs), jnp.float32),
        in_specs=[VMEM] * len(parts),
        out_specs=VMEM,
        compiler_params=grant(2),
        name="finish",
    )(*parts)


def shards(fields, weights, pair_slots, pair_counts, requests, eofs):
    lat_count, lon_count = lax.axis_size("lat"), lax.axis_size("lon")
    planes = lon_count // CORES
    requests = stay(requests.transpose(0, 2, 1))
    pair_slots = stay(pair_slots.transpose(0, 2, 1))
    pair_counts = stay(pair_counts)
    eofs = stay(eofs)
    on_chip = [(i, i ^ 1) for i in range(lon_count)]
    off_chip = [(i, (i + 2 * (i % CORES) - 1) % lon_count) for i in range(lon_count)]
    picked, later = lax.optimization_barrier((pick(requests, stay(fields)), fields))
    tiles = lax.ppermute(picked, "lon", off_chip)
    others = lax.ppermute(later, "lon", on_chip)
    grids, tile_total, pairs, cells, cells_x = weights.shape
    weights = stay(weights.reshape(grids, tile_total, pairs * cells, cells_x))
    tables = (requests, pair_slots, pair_counts, weights, eofs, fields.shape[1])
    last, spread = fold(*tables, grids - 1, 1)
    spread = lax.ppermute(spread, "lon", off_chip)
    folded, near_part, kept = fold(*tables, 0, grids - 1, (fields, others, last))
    keep, send = far(near_part, tiles, kept, folded, spread)
    pair_sum = keep + lax.ppermute(send, "lon", on_chip)
    plane_sum = pair_sum[0]
    for r in reversed(range(1, planes)):
        swap = [(i, i ^ (r * CORES)) for i in range(lon_count)]
        sent = lax.ppermute(pair_sum[r].astype(jnp.bfloat16), "lon", swap)
        plane_sum = plane_sum + sent.astype(jnp.float32)
    rows = plane_sum.shape[0] // lat_count
    parts = [plane_sum[:rows]]
    for q in reversed(range(1, lat_count)):
        swap = [(i, i ^ q) for i in range(lat_count)]
        parts.append(lax.ppermute(plane_sum[q * rows : (q + 1) * rows], "lat", swap))
    return finish(parts, eofs.shape[0]).T


def solution(mesh):
    return jax.shard_map(
        shards,
        mesh=mesh,
        in_specs=(
            P(None, ("lat", "lon"), None, None),
            P(None, ("lat", "lon"), None, None, None),
            P(None, ("lat", "lon"), None),
            P(None, ("lat", "lon")),
            P(),
            P(None, ("lat", "lon")),
        ),
        out_specs=P(None, ("lat", "lon")),
        check_vma=False,
    )
```
